256 devices in a mesh: dp: 16 (over y, x), tensor: 16 (over z, core).
Axes of the slice: x: 4, y: 4, z: 8, core: 2. Of those that a mesh axis runs over, the one named last changes fastest.
Arguments:
- tokens: bfloat16 [4096, 2048], P('dp'), may hold values from -6 to 6
- gate_weight: bfloat16 [8, 2048, 2816], P(None, 'dp', 'tensor'), may hold values from -0.25 to 0.25
- up_weight: bfloat16 [8, 2048, 2816], P(None, 'dp', 'tensor'), may hold values from -0.25 to 0.25
- down_weight: bfloat16 [8, 2816, 2048], P(None, 'tensor', 'dp'), may hold values from -0.3125 to 0.3125
- router_weight: float32 [2048, 8], replicated, may hold values from -6 to 6
- carry_mean: float32 [2048], replicated, may hold values from -0.375 to 0.375
Outputs:
- mixed: bfloat16 [4096, 2048], P(('dp', 'tensor'))
The draws below stay inside these ranges and needn't reach their ends.
All inputs are finite; a program needn't handle non-finite values.
Results may differ from the reference program's by a relative error of at most 0.028.
Values may be sent and summed in bfloat16 or wider, within the bound.
A program may use at most 64 MiB of HBM per device.

```python
import jax
import jax.numpy as jnp
from jax import lax

D = 2048
FF = 2816
EXPERTS = 8
SEG = 256
SEGMENTS = 16
TOKENS = 4096
N_DP = 16
N_TENSOR = 16


def steps_of(key, dims, shards, least, top_value):
    def one(position, shards_of):
        heights = jax.random.uniform(jax.random.fold_in(jax.random.fold_in(key, 6), position), (shards_of,), jnp.float32, least / len(shards), top_value / len(shards))
        return jnp.repeat(jnp.exp(heights), dims[position] // shards_of).reshape((-1,) + (1,) * (len(dims) - position - 1))

    level = one(*shards[0])
    for cut in shards[1:]:
        level = level * one(*cut)
    return level


def scatter_about(key, shape, width, reach, pieces=(), held_as=jnp.bfloat16):
    values = jax.random.normal(key, shape, jnp.float32) * width
    if len(pieces) > 0:
        values = steps_of(key, shape, pieces, -0.22, 0.18) * values
    return jnp.clip(values, min=-reach, max=reach).astype(held_as)


def setup_inputs(seed: int = 0) -> dict:
    key_of = jax.random.split(jax.random.key(seed), 7)
    tokens = scatter_about(key_of[0], (TOKENS, D), 1.0, 6.0, ((0, 16),))
    gate_weight = scatter_about(key_of[1], (EXPERTS, D, FF), (D // 4) ** -0.5, 0.25, ((1, 16), (2, 16)))
    up_weight = scatter_about(key_of[2], (EXPERTS, D, FF), (D // 4) ** -0.5, 0.25, ((1, 16), (2, 16)))
    down_weight = scatter_about(key_of[3], (EXPERTS, FF, D), (FF // 8) ** -0.5, 0.3125, ((1, 16), (2, 16)))
    router_weight = scatter_about(key_of[4], (D, EXPERTS), 1.0, 6.0, (), jnp.float32)
    carry_mean = scatter_about(key_of[5], (D,), 0.0625, 0.375, (), jnp.float32)
    return {"tokens": tokens, "gate_weight": gate_weight, "up_weight": up_weight, "down_weight": down_weight, "router_weight": router_weight, "carry_mean": carry_mean}


soft_cap = 8.0


def merge_rows(probs_row, weight):
    flat = weight.reshape(weight.shape[0], -1)
    merged = jnp.dot(probs_row[None, :], flat, preferred_element_type=jnp.float32)
    return merged.reshape(weight.shape[1:]).astype(jnp.bfloat16)


def blocked_product(left, right, blocks):
    rows, inner = left.shape
    outer = right.shape[1]
    left_blocks = left.astype(jnp.float32).reshape(rows, blocks, inner // blocks)
    right_blocks = right.astype(jnp.float32).reshape(blocks, inner // blocks, outer)
    parts = jnp.einsum('tkr,krf->ktf', left_blocks, right_blocks)
    rounded = lax.optimization_barrier(parts.astype(jnp.bfloat16))
    return jnp.sum(rounded.astype(jnp.float32), axis=0)


def reference(tokens, gate_weight, up_weight, down_weight, router_weight, carry_mean):
    segment_rows = tokens.reshape(SEGMENTS, SEG, D)
    segment_means = jnp.sum(segment_rows.astype(jnp.float32), axis=1) / SEG
    prior_means = jnp.concatenate([carry_mean[None, :], segment_means[:-1]], axis=0)
    raw_logits = jnp.dot(prior_means, router_weight, precision=lax.Precision.HIGHEST, preferred_element_type=jnp.float32)
    logits = soft_cap * jnp.tanh(raw_logits / soft_cap)
    scores = jnp.exp(logits)
    probs = scores / jnp.sum(scores, axis=1, keepdims=True)
    probs_bf = probs.astype(jnp.bfloat16)

    def one_segment(inputs):
        rows, probs_row = inputs
        merged_gate = merge_rows(probs_row, gate_weight)
        merged_up = merge_rows(probs_row, up_weight)
        merged_down = merge_rows(probs_row, down_weight)
        gate = blocked_product(rows, merged_gate, N_DP)
        up = blocked_product(rows, merged_up, N_DP)
        hidden = (jax.nn.silu(gate) * up).astype(jnp.bfloat16)
        mixed = blocked_product(hidden, merged_down, N_TENSOR)
        return mixed.astype(jnp.bfloat16)

    outputs = lax.map(one_segment, (segment_rows, probs_bf))
    return outputs.reshape(TOKENS, D)
```

```python
import functools

import jax
import jax.numpy as jnp
from jax import lax
from jax.experimental import pallas as pl
from jax.experimental.pallas import tpu as pltpu
from jax.sharding import PartitionSpec as P

MESH = pl.DeviceIdType.MESH
SEG = 256
CAP = 8.0
NX = 4
LANES = 128
STEP = 32

OFFSETS = (
    (2, 2), (2, 1), (2, 3), (1, 2), (3, 2), (2, 0), (0, 2),
    (1, 1), (3, 3), (1, 3), (3, 1), (1, 0), (3, 0), (0, 1), (0, 3),
)
Z_ORDER = (4, 3, 5, 2, 6, 1, 7, 0)


def kernel(
    n_dp, n_tensor,
    tok_h, gate_h, up_h, down_h, router_h, carry_h, out_ref,
    tok, weights, router, carry, row_out, row_in, prior, lhs, merged, recv,
    acc_g, acc_u, part, sib, ring_in, ring_out,
    load_sem, row_send, row_recv, gu_send, gu_recv, dn_send, dn_recv,
    sib_send, sib_recv, ring_send, ring_recv,
):
    d = lax.axis_index("dp")
    t = lax.axis_index("tensor")
    n_y = n_dp // NX
    n_z = n_tensor // 2
    x, y = lax.rem(d, NX), lax.div(d, NX)
    c, z = lax.rem(t, 2), lax.div(t, 2)
    experts = weights.shape[0]
    ff = gate_h.shape[1]

    def peer(dx, dy):
        return lax.rem(y + dy, n_y) * NX + lax.rem(x + dx, NX)

    def source(dx, dy):
        return peer(NX - dx, n_y - dy)

    def z_at(offset):
        return lax.rem(z + offset + n_z, n_z)

    sibling = z * 2 + 1 - c
    z_next = {1: z_at(1) * 2 + c, -1: z_at(-1) * 2 + c}

    loads = [
        pltpu.make_async_copy(router_h, router, load_sem.at[0]),
        pltpu.make_async_copy(carry_h, carry, load_sem.at[1]),
        pltpu.make_async_copy(tok_h, tok, load_sem.at[2]),
        pltpu.make_async_copy(gate_h, weights.at[:, 0:ff, :], load_sem.at[3]),
        pltpu.make_async_copy(up_h, weights.at[:, ff : 2 * ff, :], load_sem.at[4]),
        pltpu.make_async_copy(down_h, weights.at[:, 2 * ff : 3 * ff, :], load_sem.at[5]),
    ]
    for load in loads:
        load.start()

    barrier = pltpu.get_barrier_semaphore()
    for dx, dy in OFFSETS:
        pl.semaphore_signal(barrier, inc=1, device_id={"dp": peer(dx, dy)}, device_id_type=MESH)
    for other in (sibling, z_next[1], z_next[-1]):
        pl.semaphore_signal(barrier, inc=1, device_id={"tensor": other}, device_id_type=MESH)

    width = experts * STEP
    spread = lax.broadcasted_iota(jnp.int32, (experts, width), 1) // STEP == lax.broadcasted_iota(
        jnp.int32, (experts, width), 0
    )

    def spread_row(acc):
        total = jnp.sum(acc, axis=1, keepdims=True)
        return jnp.sum(jnp.where(spread, total, 0.0), axis=0, keepdims=True)

    loads[0].wait()
    loads[1].wait()
    blocks = tok.shape[1] // LANES
    acc = jnp.zeros((experts, LANES), jnp.float32)
    for i in range(blocks):
        acc += router[:, i * LANES : (i + 1) * LANES] * carry[i : i + 1, :]
    prior[0:1, :] = spread_row(acc)
    loads[2].wait()
    acc = jnp.zeros((experts, LANES), jnp.float32)
    for i in range(blocks):
        block = tok[:, i * LANES : (i + 1) * LANES].astype(jnp.float32)
        mean = jnp.sum(block, axis=0, keepdims=True) / SEG
        acc += router[:, i * LANES : (i + 1) * LANES] * mean
    own_row = spread_row(acc)
    row_out[...] = own_row
    row_in[d] = own_row

    pl.semaphore_wait(barrier, len(OFFSETS) + 3)

    rows = []
    for j, (dx, dy) in enumerate(OFFSETS):
        rows.append(
            pltpu.make_async_remote_copy(
                src_ref=row_out,
                dst_ref=row_in.at[d],
                send_sem=row_send.at[j],
                recv_sem=row_recv.at[j],
                device_id={"dp": peer(dx, dy)},
                device_id_type=MESH,
            )
        )
        rows[-1].start()
    for load in loads[3:]:
        load.wait()
    for copy in rows:
        copy.wait_recv()

    for s in range(n_dp - 1):
        prior[s + 1 : s + 2, :] = row_in[s]
    scores = jnp.exp(CAP * jnp.tanh(prior[...] / CAP))
    probs = scores / (jnp.sum(scores, axis=1, keepdims=True) / STEP)
    probs = probs.astype(jnp.bfloat16).astype(jnp.float32)
    diag = lax.rem(lax.broadcasted_iota(jnp.int32, (STEP, width), 1), STEP) == lax.broadcasted_iota(
        jnp.int32, (STEP, width), 0
    )
    for s in range(n_dp):
        lhs[s * STEP : (s + 1) * STEP, :] = jnp.where(diag, probs[s : s + 1, :], 0.0).astype(
            jnp.bfloat16
        )

    def merge(start):
        right = weights[:, start : start + STEP, :].reshape(width, LANES)
        both = jnp.dot(lhs[...], right, preferred_element_type=jnp.float32)
        merged[:, start : start + STEP, :] = both.astype(jnp.bfloat16).reshape(n_dp, STEP, LANES)

    def send_blocks(low, high, send_sem, recv_sem):
        copies = []
        for j, (dx, dy) in enumerate(OFFSETS):
            to = peer(dx, dy)
            copies.append(
                pltpu.make_async_remote_copy(
                    src_ref=merged.at[to, low:high, :],
                    dst_ref=recv.at[d, low:high, :],
                    send_sem=send_sem.at[j],
                    recv_sem=recv_sem.at[j],
                    device_id={"dp": to},
                    device_id_type=MESH,
                )
            )
            copies[-1].start()
        return copies

    for start in range(0, 2 * ff, STEP):
        merge(start)
    gu = send_blocks(0, 2 * ff, gu_send, gu_recv)
    starts = list(range(2 * ff, 3 * ff - STEP + 1, STEP))
    if starts[-1] + STEP < 3 * ff:
        starts.append(3 * ff - STEP)
    for start in starts:
        merge(start)
    dn = send_blocks(2 * ff, 3 * ff, dn_send, dn_recv)
    recv[d] = merged[d]

    own_first = [None] + list(range(len(OFFSETS) - 1, -1, -1))
    groups = [own_first[i : i + 4] for i in range(0, len(own_first), 4)]
    nt = (((1,), (1,)), ((), ()))
    for g, group in enumerate(groups):
        left, right_g, right_u = [], [], []
        for j in group:
            if j is None:
                src = d
            else:
                gu[j].wait_recv()
                src = source(*OFFSETS[j])
            left.append(tok[:, pl.ds(pl.multiple_of(src * LANES, LANES), LANES)])
            right_g.append(recv[src, 0:ff, :])
            right_u.append(recv[src, ff : 2 * ff, :])
        left = jnp.concatenate(left, axis=1)
        more_g = lax.dot_general(
            left, jnp.concatenate(right_g, axis=1), nt, preferred_element_type=jnp.float32
        )
        more_u = lax.dot_general(
            left, jnp.concatenate(right_u, axis=1), nt, preferred_element_type=jnp.float32
        )
        if g == 0:
            acc_g[...] = more_g
            acc_u[...] = more_u
        else:
            acc_g[...] += more_g
            acc_u[...] += more_u
    gate = acc_g[...]
    hidden = (gate / (1.0 + jnp.exp(-gate)) * acc_u[...]).astype(jnp.bfloat16)

    for copy in dn:
        copy.wait_recv()
    for i in range(0, n_dp, 2):
        right = jnp.concatenate(
            [recv[i, 2 * ff : 3 * ff, :], recv[i + 1, 2 * ff : 3 * ff, :]], axis=1
        )
        term = jnp.dot(hidden, right, preferred_element_type=jnp.float32)
        part[:, :, i * LANES : (i + 2) * LANES] = term.astype(jnp.bfloat16).reshape(
            n_tensor, SEG // n_tensor, 2 * LANES
        )

    pair = {}
    for offset in Z_ORDER:
        pair[offset] = pltpu.make_async_remote_copy(
            src_ref=part.at[z_at(offset) * 2 + 1 - c],
            dst_ref=sib.at[offset],
            send_sem=sib_send.at[offset],
            recv_sem=sib_recv.at[offset],
            device_id={"tensor": sibling},
            device_id_type=MESH,
        )
        pair[offset].start()
    half = part.shape[2] // 2
    waited = set()

    def own(offset, h):
        offset = offset % n_z
        if offset not in waited:
            pair[offset].wait_recv()
            waited.add(offset)
        cols = slice(h * half, (h + 1) * half)
        mine = part[z_at(offset) * 2 + c, :, cols].astype(jnp.float32)
        return mine + sib[offset, :, cols].astype(jnp.float32)

    far = n_z // 2
    chains = [(0, 1, far), (1, -1, far), (0, -1, far - 1), (1, 1, far - 1)]
    ring = {}
    for k in range(far):
        for i, (h, way, length) in enumerate(chains):
            if k >= length:
                continue
            value = own(way * (length - k), h)
            if k:
                ring[i, k - 1].wait_recv()
                value = value + ring_in[i, k - 1].astype(jnp.float32)
            ring_out[i, k] = value.astype(jnp.bfloat16)
            ring[i, k] = pltpu.make_async_remote_copy(
                src_ref=ring_out.at[i, k],
                dst_ref=ring_in.at[i, k],
                send_sem=ring_send.at[i, k],
                recv_sem=ring_recv.at[i, k],
                device_id={"tensor": z_next[way]},
                device_id_type=MESH,
            )
            ring[i, k].start()
    for h in range(2):
        value = own(0, h)
        for i, (of, way, length) in enumerate(chains):
            if of == h:
                ring[i, length - 1].wait_recv()
                value = value + ring_in[i, length - 1].astype(jnp.float32)
        out_ref[:, h * half : (h + 1) * half] = value.astype(jnp.bfloat16)

    for copy in rows + gu + dn + list(pair.values()) + list(ring.values()):
        copy.wait_send()


def solution(mesh):
    n_dp, n_tensor = mesh.shape["dp"], mesh.shape["tensor"]

    def on_device(tokens, gate_weight, up_weight, down_weight, router_weight, carry_mean):
        rows, width = tokens.shape
        experts, _, ff = gate_weight.shape
        n_z = n_tensor // 2
        peers = len(OFFSETS)
        block = rows // n_tensor
        any_space = pl.BlockSpec(memory_space=pl.ANY)
        bf16, f32 = jnp.bfloat16, jnp.float32
        dma = pltpu.SemaphoreType.DMA
        return pl.pallas_call(
            functools.partial(kernel, n_dp, n_tensor),
            out_shape=jax.ShapeDtypeStruct((block, width), bf16),
            in_specs=[any_space] * 6,
            out_specs=pl.BlockSpec(memory_space=pltpu.VMEM),
            scratch_shapes=[
                pltpu.VMEM((rows, width), bf16),
                pltpu.VMEM((experts, 3 * ff, LANES), bf16),
                pltpu.VMEM((experts, width), f32),
                pltpu.VMEM((width // LANES, LANES), f32),
                pltpu.VMEM((1, experts * STEP), f32),
                pltpu.VMEM((n_dp, 1, experts * STEP), f32),
                pltpu.VMEM((n_dp, experts * STEP), f32),
                pltpu.VMEM((n_dp * STEP, experts * STEP), bf16),
                pltpu.VMEM((n_dp, 3 * ff, LANES), bf16),
                pltpu.VMEM((n_dp, 3 * ff, LANES), bf16),
                pltpu.VMEM((rows, ff), f32),
                pltpu.VMEM((rows, ff), f32),
                pltpu.VMEM((n_tensor, block, width), bf16),
                pltpu.VMEM((n_z, block, width), bf16),
                pltpu.VMEM((4, n_z // 2, block, width // 2), bf16),
                pltpu.VMEM((4, n_z // 2, block, width // 2), bf16),
                dma((6,)),
                dma((peers,)), dma((peers,)),
                dma((peers,)), dma((peers,)),
                dma((peers,)), dma((peers,)),
                dma((n_z,)), dma((n_z,)),
                dma((4, n_z // 2)), dma((4, n_z // 2)),
            ],
            compiler_params=pltpu.CompilerParams(
                collective_id=0, has_side_effects=True, vmem_limit_bytes=67043328
            ),
        )(
            tokens,
            jnp.transpose(gate_weight, (0, 2, 1)),
            jnp.transpose(up_weight, (0, 2, 1)),
            down_weight,
            router_weight.T,
            carry_mean.reshape(width // LANES, LANES),
        )

    placed = (
        P("dp", None),
        P(None, "dp", "tensor"),
        P(None, "dp", "tensor"),
        P(None, "tensor", "dp"),
        P(),
        P(),
    )
    return jax.shard_map(
        on_device, mesh=mesh, in_specs=placed, out_specs=P(("dp", "tensor"), None), check_vma=False
    )
```

```python
import functools

import jax
import jax.numpy as jnp
from jax import lax
from jax.experimental import pallas as pl
from jax.experimental.pallas import tpu as pltpu
from jax.sharding import PartitionSpec as P

MESH = pl.DeviceIdType.MESH
SEG = 256
CAP = 8.0
NX = 4
LANES = 128
STEP = 32

READY = (
    ((1, 0), (2, 0), (1, 1), (1, 3)),
    ((3, 0), (0, 1), (0, 3), (2, 1), (2, 3), (1, 2)),
    ((3, 1), (3, 3), (0, 2), (2, 2), (3, 2), (0, 0)),
)
OFFSETS = tuple(o for group in READY for o in group if o != (0, 0))
ALL = OFFSETS + ((0, 0),)
SLOTS = (((0, 0), (1, 2)), ((0, 2), (1, 0)), ((0, 1), (1, 3)), ((0, 3), (1, 1)))


def kernel(
    n_dp, n_tensor,
    tok_h, gate_h, up_h, down_h, router_h, carry_h, out_ref,
    tok, weights, router, carry, row_out, row_in, merged, recv, recv_dn,
    acc_g, acc_u, hid, part, ring_in, ring_out, fin_in, sib_out, sib_in,
    load_sem, row_send, row_recv, gu_send, gu_recv, dn_send, dn_recv, own_send,
    hid_send, hid_recv, ring_send, ring_recv, fin_send, fin_recv, sib_send, sib_recv,
):
    d = lax.axis_index("dp")
    t = lax.axis_index("tensor")
    n_y = n_dp // NX
    n_z = n_tensor // 2
    x, y = lax.rem(d, NX), lax.div(d, NX)
    c, z = lax.rem(t, 2), lax.div(t, 2)
    q = lax.rem(x + c, 2)
    experts = weights.shape[0]
    ff = gate_h.shape[1]

    def peer(dx, dy):
        return lax.rem(y + dy, n_y) * NX + lax.rem(x + dx, NX)

    def source(dx, dy):
        return lax.rem(y + n_y - dy, n_y) * NX + lax.rem(x + NX - dx, NX)

    def z_at(offset):
        return lax.rem(z + offset + n_z, n_z)

    sibling = z * 2 + 1 - c

    def copy_to(src, dst, send, recv_sem, dp=None, tensor=None):
        to = {}
        if dp is not None:
            to["dp"] = dp
        if tensor is not None:
            to["tensor"] = tensor
        return pltpu.make_async_remote_copy(
            src_ref=src, dst_ref=dst, send_sem=send, recv_sem=recv_sem,
            device_id=to, device_id_type=MESH,
        )

    loads = [
        pltpu.make_async_copy(router_h, router, load_sem.at[0]),
        pltpu.make_async_copy(carry_h, carry, load_sem.at[1]),
        pltpu.make_async_copy(tok_h, tok, load_sem.at[2]),
        pltpu.make_async_copy(gate_h, weights.at[:, 0:ff, :], load_sem.at[3]),
        pltpu.make_async_copy(up_h, weights.at[:, ff : 2 * ff, :], load_sem.at[4]),
        pltpu.make_async_copy(down_h, weights.at[:, 2 * ff : 3 * ff, :], load_sem.at[5]),
    ]
    for load in loads:
        load.start()

    barrier = pltpu.get_barrier_semaphore()
    greeted = 0
    for dx, dy in OFFSETS:
        for tensor in (t, sibling):
            pl.semaphore_signal(
                barrier, inc=1, device_id={"dp": peer(dx, dy), "tensor": tensor}, device_id_type=MESH
            )
            greeted += 1
    for tensor in (sibling, *(z_at(way) * 2 + core for way in (1, -1) for core in (0, 1))):
        pl.semaphore_signal(barrier, inc=1, device_id={"tensor": tensor}, device_id_type=MESH)
        greeted += 1

    width = experts * STEP
    spread = lax.broadcasted_iota(jnp.int32, (experts, width), 1) // STEP == lax.broadcasted_iota(
        jnp.int32, (experts, width), 0
    )
    for load in loads[:3]:
        load.wait()
    acc = jnp.zeros((experts, LANES), jnp.float32)
    for i in range(tok.shape[1] // LANES):
        block = tok[:, i * LANES : (i + 1) * LANES].astype(jnp.float32)
        mean = jnp.sum(block, axis=0, keepdims=True) / SEG
        mean = jnp.where(d == n_dp - 1, carry[i : i + 1, :], mean)
        acc += router[:, i * LANES : (i + 1) * LANES] * mean
    total = jnp.sum(acc, axis=1, keepdims=True)
    logits = CAP * jnp.tanh(total / CAP)
    scores = jnp.exp(logits)
    probs = scores / jnp.sum(scores, axis=0, keepdims=True)
    probs = probs.astype(jnp.bfloat16).astype(jnp.float32)
    own_row = jnp.sum(jnp.where(spread, probs, 0.0), axis=0, keepdims=True)
    row_out[...] = own_row
    row_in[d] = own_row

    pl.semaphore_wait(barrier, greeted)

    rows = []
    for j, (dx, dy) in enumerate(OFFSETS):
        rows.append(
            copy_to(row_out, row_in.at[d], row_send.at[j], row_recv.at[d], dp=peer(dx, dy))
        )
        rows[-1].start()
    for load in loads[3:]:
        load.wait()

    diag = lax.rem(lax.broadcasted_iota(jnp.int32, (STEP, width), 1), STEP) == lax.broadcasted_iota(
        jnp.int32, (STEP, width), 0
    )

    def merge(left, first, start):
        count = left.shape[0] // STEP
        right = weights[:, start : start + STEP, :].reshape(width, LANES)
        both = jnp.dot(left, right, preferred_element_type=jnp.float32)
        merged[first : first + count, start : start + STEP, :] = both.astype(jnp.bfloat16).reshape(
            count, STEP, LANES
        )

    gu = []
    lefts = []
    for group in READY:
        left = []
        for dx, dy in group:
            src = lax.rem(peer(dx, dy) + n_dp - 1, n_dp)

            @pl.when(src != d)
            def _():
                copy_to(row_out, row_in.at[src], row_send.at[0], row_recv.at[src], dp=src).wait_recv()

            left.append(jnp.where(diag, row_in[src], 0.0).astype(jnp.bfloat16))
        left = jnp.concatenate(left, axis=0)
        first = ALL.index(group[0])
        lefts.append((left, first))
        for start in range(0, 2 * ff, STEP):
            merge(left, first, start)
        for offset in group:
            if offset == (0, 0):
                continue
            j = OFFSETS.index(offset)
            gu.append(
                copy_to(
                    merged.at[j, 0 : 2 * ff, :], recv.at[j], gu_send.at[j], gu_recv.at[j],
                    dp=peer(*offset),
                )
            )
            gu[-1].start()

    starts = list(range(2 * ff, 3 * ff - STEP + 1, STEP))
    if starts[-1] + STEP < 3 * ff:
        starts.append(3 * ff - STEP)
    for left, first in lefts:
        for start in starts:
            merge(left, first, start)
    own_at = len(OFFSETS)
    half_rows = pl.ds(pl.multiple_of(c * ff, 16), ff)
    dn = {}
    for g, group in enumerate(SLOTS):
        for s, (a, dy) in enumerate(group):
            slot = 2 * g + s
            for dx in (2 * a, 2 * a + 1):
                if (dx, dy) == (0, 0):
                    continue
                j = OFFSETS.index((dx, dy))
                dn[dx, dy] = copy_to(
                    merged.at[j, 2 * ff : 3 * ff, :], recv_dn.at[slot, half_rows, :],
                    dn_send.at[j], dn_recv.at[slot, c],
                    dp=peer(dx, dy), tensor=z * 2 + lax.rem(x, 2),
                )
                dn[dx, dy].start()
    own_copy = copy_to(
        merged.at[own_at, 2 * ff : 3 * ff, :], recv_dn.at[0, half_rows, :],
        own_send, dn_recv.at[0, c], tensor=sibling,
    )

    @pl.when(q == 1)
    def _():
        own_copy.start()

    @pl.when(q == 0)
    def _():
        recv_dn[0, half_rows, :] = merged[own_at, 2 * ff : 3 * ff, :]

    order = [own_at] + list(range(len(OFFSETS)))
    nt = (((1,), (1,)), ((), ()))
    for g in range(0, len(order), 4):
        left, right_g, right_u = [], [], []
        for j in order[g : g + 4]:
            if j == own_at:
                src, block = d, merged.at[own_at]
            else:
                gu[j].wait_recv()
                src, block = source(*OFFSETS[j]), recv.at[j]
            left.append(tok[:, pl.ds(pl.multiple_of(src * LANES, LANES), LANES)])
            right_g.append(block[0:ff, :])
            right_u.append(block[ff : 2 * ff, :])
        left = jnp.concatenate(left, axis=1)
        more_g = lax.dot_general(
            left, jnp.concatenate(right_g, axis=1), nt, preferred_element_type=jnp.float32
        )
        more_u = lax.dot_general(
            left, jnp.concatenate(right_u, axis=1), nt, preferred_element_type=jnp.float32
        )
        if g == 0:
            acc_g[...] = more_g
            acc_u[...] = more_u
        else:
            acc_g[...] += more_g
            acc_u[...] += more_u
    gate = acc_g[...]
    hid[c] = (gate / (1.0 + jnp.exp(-gate)) * acc_u[...]).astype(jnp.bfloat16)
    swap = copy_to(hid.at[c], hid.at[c], hid_send, hid_recv, tensor=sibling)
    swap.start()
    swap.wait_recv()

    far = n_z // 2
    block = part.shape[2] // 2
    cols = part.shape[3]
    ring, fin, sib = {}, {}, {}

    def length(g, w):
        return far - (g + w) % 2

    def link(g, w, k):
        way = 1 - 2 * w
        last = length(g, w) - 1
        value = part[g, z_at(way * (last + 1 - k))]
        if k:
            ring[g, w, k - 1].wait_recv()
            value = value + ring_in[g, w, k - 1].astype(jnp.float32)
        ring_out[g, w, k] = value.astype(jnp.bfloat16)
        if k < last:
            ring[g, w, k] = copy_to(
                ring_out.at[g, w, k], ring_in.at[g, w, k],
                ring_send.at[g, w, k], ring_recv.at[g, w, k], tensor=z_at(way) * 2 + c,
            )
            ring[g, w, k].start()
        else:
            for core in range(2):
                fin[g, w, core] = copy_to(
                    ring_out.at[g, w, k, core * block : (core + 1) * block, :],
                    fin_in.at[g, w, c],
                    fin_send.at[g, w, core], fin_recv.at[g, w, c], tensor=z_at(way) * 2 + core,
                )
                fin[g, w, core].start()

    def begin(g):
        for s, (a, dy) in enumerate(SLOTS[g]):
            slot = 2 * g + s
            low = copy_to(
                merged.at[0, 2 * ff : 3 * ff, :], recv_dn.at[slot, 0:ff, :],
                dn_send.at[0], dn_recv.at[slot, 0], tensor=sibling,
            )
            high = copy_to(
                merged.at[0, 2 * ff : 3 * ff, :], recv_dn.at[slot, ff : 2 * ff, :],
                dn_send.at[0], dn_recv.at[slot, 1], tensor=sibling,
            )
            if slot:
                low.wait_recv()
                high.wait_recv()
            else:

                @pl.when((q == 1) | (c == 1))
                def _():
                    low.wait_recv()

                @pl.when((q == 1) | (c == 0))
                def _():
                    high.wait_recv()

        term = None
        for core in range(2):
            right = jnp.concatenate(
                [recv_dn[2 * g + s, core * ff : (core + 1) * ff, :] for s in range(2)], axis=1
            )
            more = jnp.dot(hid[core], right, preferred_element_type=jnp.float32)
            term = more if term is None else term + more
        part[g] = term.reshape(n_z, 2 * block, cols)

    def to_sibling(g):
        other = pl.ds(pl.multiple_of((1 - c) * block, block), block)
        sib_out[g] = part[g, z, other, :].astype(jnp.bfloat16)
        sib[g] = copy_to(
            sib_out.at[g], sib_in.at[g], sib_send.at[g], sib_recv.at[g], tensor=sibling
        )
        sib[g].start()

    n_groups = len(SLOTS)
    for tick in range(n_groups + far):
        if tick < n_groups:
            begin(tick)
        for g in range(min(tick, n_groups - 1), -1, -1):
            k = tick - g
            for w in (g % 2, 1 - g % 2):
                if k < length(g, w):
                    link(g, w, k)
            if k == 0:
                to_sibling(g)

    mine = pl.ds(pl.multiple_of(c * block, block), block)
    for g in range(n_groups):
        sib[g].wait_recv()
        from_core = [part[g, z, mine, :], sib_in[g].astype(jnp.float32)]
        for of in range(2):
            core = c if of == 0 else 1 - c
            value = from_core[of]
            for w in range(2):
                copy_to(
                    sib_out.at[g], fin_in.at[g, w, core],
                    fin_send.at[g, w, 0], fin_recv.at[g, w, core], tensor=sibling,
                ).wait_recv()
                value = value + fin_in[g, w, core].astype(jnp.float32)
            odd = lax.rem(x + core, 2)
            for s, (a, dy) in enumerate(SLOTS[g]):
                src = source(2 * a + odd, dy)
                out_ref[:, pl.ds(pl.multiple_of(src * LANES, LANES), LANES)] = value[
                    :, s * LANES : (s + 1) * LANES
                ].astype(jnp.bfloat16)

    for copy in rows + gu + list(dn.values()):
        copy.wait_send()

    @pl.when(q == 1)
    def _():
        own_copy.wait_send()

    swap.wait_send()
    for copies in (ring, fin, sib):
        for copy in copies.values():
            copy.wait_send()


def solution(mesh):
    n_dp, n_tensor = mesh.shape["dp"], mesh.shape["tensor"]

    def on_device(tokens, gate_weight, up_weight, down_weight, router_weight, carry_mean):
        rows, width = tokens.shape
        experts, _, ff = gate_weight.shape
        n_z = n_tensor // 2
        peers = len(OFFSETS)
        groups = len(SLOTS)
        block = rows // n_tensor
        cols = 2 * LANES
        bf16, f32 = jnp.bfloat16, jnp.float32
        dma = pltpu.SemaphoreType.DMA
        return pl.pallas_call(
            functools.partial(kernel, n_dp, n_tensor),
            out_shape=jax.ShapeDtypeStruct((block, width), bf16),
            in_specs=[pl.BlockSpec(memory_space=pltpu.HBM)] * 6,
            out_specs=pl.BlockSpec(memory_space=pltpu.VMEM),
            scratch_shapes=[
                pltpu.VMEM((rows, width), bf16),
                pltpu.VMEM((experts, 3 * ff, LANES), bf16),
                pltpu.VMEM((experts, width), f32),
                pltpu.VMEM((width // LANES, LANES), f32),
                pltpu.VMEM((1, experts * STEP), f32),
                pltpu.VMEM((n_dp, 1, experts * STEP), f32),
                pltpu.VMEM((n_dp, 3 * ff, LANES), bf16),
                pltpu.VMEM((peers, 2 * ff, LANES), bf16),
                pltpu.VMEM((n_dp // 2, 2 * ff, LANES), bf16),
                pltpu.VMEM((rows, ff), f32),
                pltpu.VMEM((rows, ff), f32),
                pltpu.VMEM((2, rows, ff), bf16),
                pltpu.VMEM((groups, n_z, 2 * block, cols), f32),
                pltpu.VMEM((groups, 2, n_z // 2, 2 * block, cols), bf16),
                pltpu.VMEM((groups, 2, n_z // 2, 2 * block, cols), bf16),
                pltpu.VMEM((groups, 2, 2, block, cols), bf16),
                pltpu.VMEM((groups, block, cols), bf16),
                pltpu.VMEM((groups, block, cols), bf16),
                dma((6,)),
                dma((peers,)), dma((n_dp,)),
                dma((peers,)), dma((peers,)),
                dma((peers,)), dma((n_dp // 2, 2)), dma(()),
                dma(()), dma(()),
                dma((groups, 2, n_z // 2)), dma((groups, 2, n_z // 2)),
                dma((groups, 2, 2)), dma((groups, 2, 2)),
                dma((groups,)), dma((groups,)),
            ],
            compiler_params=pltpu.CompilerParams(
                collective_id=0, has_side_effects=True, vmem_limit_bytes=67043328
            ),
        )(
            tokens,
            jnp.transpose(gate_weight, (0, 2, 1)),
            jnp.transpose(up_weight, (0, 2, 1)),
            down_weight,
            router_weight.T,
            carry_mean.reshape(width // LANES, LANES),
        )

    placed = (
        P("dp", None),
        P(None, "dp", "tensor"),
        P(None, "dp", "tensor"),
        P(None, "tensor", "dp"),
        P(),
        P(),
    )
    return jax.shard_map(
        on_device, mesh=mesh, in_specs=placed, out_specs=P(("dp", "tensor"), None), check_vma=False
    )
```

```python
import functools

import jax
import jax.numpy as jnp
from jax import lax
from jax.experimental import pallas as pl
from jax.experimental.pallas import tpu as pltpu
from jax.sharding import PartitionSpec as P

MESH = pl.DeviceIdType.MESH
SEG = 256
CAP = 8.0
NX = 4
LANES = 128
STEP = 32

READY = (
    ((2, 2), (2, 1), (2, 3), (1, 2), (3, 2), (2, 0), (0, 2), (1, 1)),
    ((3, 3), (1, 3), (3, 1), (1, 0), (3, 0), (0, 1), (0, 3), (0, 0)),
)
OFFSETS = tuple(o for group in READY for o in group if o != (0, 0))
ALL = OFFSETS + ((0, 0),)
Z_ORDER = (4, 3, 5, 2, 6, 1, 7, 0)
SLOTS = (((0, 0), (1, 2)), ((0, 2), (1, 0)), ((0, 1), (1, 3)), ((0, 3), (1, 1)))


def kernel(
    n_dp, n_tensor,
    tok_h, gate_h, up_h, down_h, router_h, carry_h, out_ref,
    tok, weights, router, carry, row_out, row_in, merged, recv, recv_dn,
    acc_g, acc_u, hid, part, red_in,
    load_sem, row_send, row_recv, gu_send, gu_recv, dn_send, dn_recv, own_send,
    hid_send, hid_recv, red_send, red_recv, round_sem,
):
    d = lax.axis_index("dp")
    t = lax.axis_index("tensor")
    n_y = n_dp // NX
    n_z = n_tensor // 2
    x, y = lax.rem(d, NX), lax.div(d, NX)
    c, z = lax.rem(t, 2), lax.div(t, 2)
    q = lax.rem(x + c, 2)
    experts = weights.shape[0]
    ff = gate_h.shape[1]

    def peer(dx, dy):
        return lax.rem(y + dy, n_y) * NX + lax.rem(x + dx, NX)

    def source(dx, dy):
        return lax.rem(y + n_y - dy, n_y) * NX + lax.rem(x + NX - dx, NX)

    def z_at(offset):
        return lax.rem(z + offset + n_z, n_z)

    sibling = z * 2 + 1 - c

    def copy_to(src, dst, send, recv_sem, dp=None, tensor=None):
        to = {}
        if dp is not None:
            to["dp"] = dp
        if tensor is not None:
            to["tensor"] = tensor
        return pltpu.make_async_remote_copy(
            src_ref=src, dst_ref=dst, send_sem=send, recv_sem=recv_sem,
            device_id=to, device_id_type=MESH,
        )

    loads = [
        pltpu.make_async_copy(router_h, router, load_sem.at[0]),
        pltpu.make_async_copy(carry_h, carry, load_sem.at[1]),
        pltpu.make_async_copy(tok_h, tok, load_sem.at[2]),
        pltpu.make_async_copy(gate_h, weights.at[:, 0:ff, :], load_sem.at[3]),
        pltpu.make_async_copy(up_h, weights.at[:, ff : 2 * ff, :], load_sem.at[4]),
        pltpu.make_async_copy(down_h, weights.at[:, 2 * ff : 3 * ff, :], load_sem.at[5]),
    ]
    for load in loads:
        load.start()

    barrier = pltpu.get_barrier_semaphore()
    for dx, dy in OFFSETS:
        pl.semaphore_signal(barrier, inc=1, device_id={"dp": peer(dx, dy)}, device_id_type=MESH)
    neighbours = [z_at(1) * 2 + c, z_at(-1) * 2 + c]
    for tensor in [sibling] + neighbours:
        pl.semaphore_signal(barrier, inc=1, device_id={"tensor": tensor}, device_id_type=MESH)

    width = experts * STEP
    spread = lax.broadcasted_iota(jnp.int32, (experts, width), 1) // STEP == lax.broadcasted_iota(
        jnp.int32, (experts, width), 0
    )
    for load in loads[:3]:
        load.wait()
    acc = jnp.zeros((experts, LANES), jnp.float32)
    for i in range(tok.shape[1] // LANES):
        block = tok[:, i * LANES : (i + 1) * LANES].astype(jnp.float32)
        mean = jnp.sum(block, axis=0, keepdims=True) / SEG
        mean = jnp.where(d == n_dp - 1, carry[i : i + 1, :], mean)
        acc += router[:, i * LANES : (i + 1) * LANES] * mean
    total = jnp.sum(acc, axis=1, keepdims=True)
    logits = CAP * jnp.tanh(total / CAP)
    scores = jnp.exp(logits)
    probs = scores / jnp.sum(scores, axis=0, keepdims=True)
    probs = probs.astype(jnp.bfloat16).astype(jnp.float32)
    own_row = jnp.sum(jnp.where(spread, probs, 0.0), axis=0, keepdims=True)
    row_out[...] = own_row
    row_in[d] = own_row

    pl.semaphore_wait(barrier, len(OFFSETS) + 3)

    rows = []
    for j, (dx, dy) in enumerate(OFFSETS):
        rows.append(
            copy_to(row_out, row_in.at[d], row_send.at[j], row_recv.at[j], dp=peer(dx, dy))
        )
        rows[-1].start()
    for load in loads[3:]:
        load.wait()

    diag = lax.rem(lax.broadcasted_iota(jnp.int32, (STEP, width), 1), STEP) == lax.broadcasted_iota(
        jnp.int32, (STEP, width), 0
    )

    def merge(left, first, start):
        count = left.shape[0] // STEP
        right = weights[:, start : start + STEP, :].reshape(width, LANES)
        both = jnp.dot(left, right, preferred_element_type=jnp.float32)
        merged[first : first + count, start : start + STEP, :] = both.astype(jnp.bfloat16).reshape(
            count, STEP, LANES
        )

    for copy in rows:
        copy.wait_recv()
    gu = []
    lefts = []
    for group in READY:
        left = []
        for dx, dy in group:
            src = lax.rem(peer(dx, dy) + n_dp - 1, n_dp)
            left.append(jnp.where(diag, row_in[src], 0.0).astype(jnp.bfloat16))
        left = jnp.concatenate(left, axis=0)
        first = ALL.index(group[0])
        lefts.append((left, first))
        for start in range(0, 2 * ff, STEP):
            merge(left, first, start)
        for offset in group:
            if offset == (0, 0):
                continue
            j = OFFSETS.index(offset)
            gu.append(
                copy_to(
                    merged.at[j, 0 : 2 * ff, :], recv.at[j], gu_send.at[j], gu_recv.at[j],
                    dp=peer(*offset),
                )
            )
            gu[-1].start()

    starts = list(range(2 * ff, 3 * ff - STEP + 1, STEP))
    if starts[-1] + STEP < 3 * ff:
        starts.append(3 * ff - STEP)
    for left, first in lefts:
        for start in starts:
            merge(left, first, start)
    own_at = len(OFFSETS)
    half_rows = pl.ds(pl.multiple_of(c * ff, 16), ff)
    dn = {}
    for g, group in enumerate(SLOTS):
        for s, (a, dy) in enumerate(group):
            slot = 2 * g + s
            for dx in (2 * a, 2 * a + 1):
                if (dx, dy) == (0, 0):
                    continue
                j = OFFSETS.index((dx, dy))
                dn[dx, dy] = copy_to(
                    merged.at[j, 2 * ff : 3 * ff, :], recv_dn.at[slot, half_rows, :],
                    dn_send.at[j], dn_recv.at[slot, c],
                    dp=peer(dx, dy), tensor=z * 2 + lax.rem(x, 2),
                )
                dn[dx, dy].start()
    own_copy = copy_to(
        merged.at[own_at, 2 * ff : 3 * ff, :], recv_dn.at[0, half_rows, :],
        own_send, dn_recv.at[0, c], tensor=sibling,
    )

    @pl.when(q == 1)
    def _():
        own_copy.start()

    @pl.when(q == 0)
    def _():
        recv_dn[0, half_rows, :] = merged[own_at, 2 * ff : 3 * ff, :]

    order = [own_at] + list(range(len(OFFSETS)))
    nt = (((1,), (1,)), ((), ()))
    for g in range(0, len(order), 4):
        for tensor in neighbours:
            pl.semaphore_signal(
                round_sem.at[g // 4], inc=1, device_id={"tensor": tensor}, device_id_type=MESH
            )
        left, right_g, right_u = [], [], []
        for j in order[g : g + 4]:
            if j == own_at:
                src, block = d, merged.at[own_at]
            else:
                gu[j].wait_recv()
                src, block = source(*OFFSETS[j]), recv.at[j]
            left.append(tok[:, pl.ds(pl.multiple_of(src * LANES, LANES), LANES)])
            right_g.append(block[0:ff, :])
            right_u.append(block[ff : 2 * ff, :])
        left = jnp.concatenate(left, axis=1)
        more_g = lax.dot_general(
            left, jnp.concatenate(right_g, axis=1), nt, preferred_element_type=jnp.float32
        )
        more_u = lax.dot_general(
            left, jnp.concatenate(right_u, axis=1), nt, preferred_element_type=jnp.float32
        )
        if g == 0:
            acc_g[...] = more_g
            acc_u[...] = more_u
        else:
            acc_g[...] += more_g
            acc_u[...] += more_u
        pl.semaphore_wait(round_sem.at[g // 4], 2)
    gate = acc_g[...]
    hid[c] = (gate / (1.0 + jnp.exp(-gate)) * acc_u[...]).astype(jnp.bfloat16)
    swap = copy_to(hid.at[c], hid.at[c], hid_send, hid_recv, tensor=sibling)
    swap.start()
    swap.wait_recv()

    block = part.shape[2]
    red = {}

    def begin(g):
        for s, (a, dy) in enumerate(SLOTS[g]):
            slot = 2 * g + s
            low = copy_to(
                merged.at[0, 2 * ff : 3 * ff, :], recv_dn.at[slot, 0:ff, :],
                dn_send.at[0], dn_recv.at[slot, 0], tensor=sibling,
            )
            high = copy_to(
                merged.at[0, 2 * ff : 3 * ff, :], recv_dn.at[slot, ff : 2 * ff, :],
                dn_send.at[0], dn_recv.at[slot, 1], tensor=sibling,
            )
            if slot:
                low.wait_recv()
                high.wait_recv()
            else:

                @pl.when((q == 1) | (c == 1))
                def _():
                    low.wait_recv()

                @pl.when((q == 1) | (c == 0))
                def _():
                    high.wait_recv()

        term = None
        for core in range(2):
            right = jnp.concatenate(
                [recv_dn[2 * g + s, core * ff : (core + 1) * ff, :] for s in range(2)], axis=1
            )
            more = jnp.dot(hid[core], right, preferred_element_type=jnp.float32)
            term = more if term is None else term + more
        part[g] = term.astype(jnp.bfloat16).reshape(n_tensor, block, part.shape[3])
        for offset in Z_ORDER:
            for core in (0, 1):
                if offset:
                    to = z_at(offset) * 2 + core
                elif core:
                    to = sibling
                else:
                    continue
                red[g, offset, core] = copy_to(
                    part.at[g, to], red_in.at[g, offset, c],
                    red_send.at[g, offset, core], red_recv.at[g, offset, c], tensor=to,
                )
                red[g, offset, core].start()

    for g in range(len(SLOTS)):
        begin(g)
    for g in range(len(SLOTS)):
        for offset in Z_ORDER:
            for core in (c, 1 - c) if offset else (1 - c,):
                copy_to(
                    part.at[g, t], red_in.at[g, offset, core],
                    red_send.at[g, 0, 0], red_recv.at[g, offset, core], tensor=sibling,
                ).wait_recv()
        for of in range(2):
            core = c if of == 0 else 1 - c
            value = (part[g, t] if of == 0 else red_in[g, 0, core]).astype(jnp.float32)
            for offset in range(1, n_z):
                value = value + red_in[g, offset, core].astype(jnp.float32)
            odd = lax.rem(x + core, 2)
            for s, (a, dy) in enumerate(SLOTS[g]):
                src = source(2 * a + odd, dy)
                out_ref[:, pl.ds(pl.multiple_of(src * LANES, LANES), LANES)] = value[
                    :, s * LANES : (s + 1) * LANES
                ].astype(jnp.bfloat16)

    for copy in rows + gu + list(dn.values()):
        copy.wait_send()

    @pl.when(q == 1)
    def _():
        own_copy.wait_send()

    swap.wait_send()
    for copy in red.values():
        copy.wait_send()


def solution(mesh):
    n_dp, n_tensor = mesh.shape["dp"], mesh.shape["tensor"]

    def on_device(tokens, gate_weight, up_weight, down_weight, router_weight, carry_mean):
        rows, width = tokens.shape
        experts, _, ff = gate_weight.shape
        n_z = n_tensor // 2
        peers = len(OFFSETS)
        groups = len(SLOTS)
        block = rows // n_tensor
        cols = 2 * LANES
        bf16, f32 = jnp.bfloat16, jnp.float32
        dma = pltpu.SemaphoreType.DMA
        return pl.pallas_call(
            functools.partial(kernel, n_dp, n_tensor),
            out_shape=jax.ShapeDtypeStruct((block, width), bf16),
            in_specs=[pl.BlockSpec(memory_space=pltpu.HBM)] * 6,
            out_specs=pl.BlockSpec(memory_space=pltpu.VMEM),
            scratch_shapes=[
                pltpu.VMEM((rows, width), bf16),
                pltpu.VMEM((experts, 3 * ff, LANES), bf16),
                pltpu.VMEM((experts, width), f32),
                pltpu.VMEM((width // LANES, LANES), f32),
                pltpu.VMEM((1, experts * STEP), f32),
                pltpu.VMEM((n_dp, 1, experts * STEP), f32),
                pltpu.VMEM((n_dp, 3 * ff, LANES), bf16),
                pltpu.VMEM((peers, 2 * ff, LANES), bf16),
                pltpu.VMEM((n_dp // 2, 2 * ff, LANES), bf16),
                pltpu.VMEM((rows, ff), f32),
                pltpu.VMEM((rows, ff), f32),
                pltpu.VMEM((2, rows, ff), bf16),
                pltpu.VMEM((groups, n_tensor, block, cols), bf16),
                pltpu.VMEM((groups, n_z, 2, block, cols), bf16),
                dma((6,)),
                dma((peers,)), dma((peers,)),
                dma((peers,)), dma((peers,)),
                dma((peers,)), dma((n_dp // 2, 2)), dma(()),
                dma(()), dma(()),
                dma((groups, n_z, 2)), dma((groups, n_z, 2)),
                pltpu.SemaphoreType.REGULAR((4,)),
            ],
            compiler_params=pltpu.CompilerParams(
                collective_id=0, has_side_effects=True, vmem_limit_bytes=32 << 20
            ),
        )(
            *(
                pltpu.with_memory_space_constraint(operand, pltpu.HBM)
                for operand in (
                    tokens,
                    jnp.transpose(gate_weight, (0, 2, 1)),
                    jnp.transpose(up_weight, (0, 2, 1)),
                    down_weight,
                    router_weight.T,
                    carry_mean.reshape(width // LANES, LANES),
                )
            )
        )

    placed = (
        P("dp", None),
        P(None, "dp", "tensor"),
        P(None, "dp", "tensor"),
        P(None, "tensor", "dp"),
        P(),
        P(),
    )
    return jax.shard_map(
        on_device, mesh=mesh, in_specs=placed, out_specs=P(("dp", "tensor"), None), check_vma=False
    )
```

```python
import functools

import jax
import jax.numpy as jnp
from jax import lax
from jax.experimental import pallas as pl
from jax.experimental.pallas import tpu as pltpu
from jax.sharding import PartitionSpec as P

MESH = pl.DeviceIdType.MESH
SEG = 256
CAP = 8.0
NX = 4
LANES = 128
STEP = 32

READY = (
    ((2, 1), (2, 3), (1, 2), (2, 0), (1, 0), (3, 0), (0, 1), (0, 3)),
    ((2, 2), (3, 2), (0, 2), (1, 1), (3, 3), (1, 3), (3, 1), (0, 0)),
)
OFFSETS = tuple(o for group in READY for o in group if o != (0, 0))
ALL = OFFSETS + ((0, 0),)
SLOTS = (((0, 0), (1, 2)), ((0, 2), (1, 0)), ((0, 1), (1, 3)), ((0, 3), (1, 1)))
SLOT_LIST = tuple(slot for group in SLOTS for slot in group)


def kernel(
    n_dp, n_tensor,
    tok_h, gate_h, up_h, down_h, router_h, carry_h, out_ref,
    tok, weights, router, carry, row_out, row_in, merged, recv, recv_dn,
    acc_g, acc_u, hid, part, via_in, via_out, red_in,
    load_sem, row_send, row_recv, gu_send, gu_recv, dn_send, dn_recv, own_send,
    hid_send, hid_recv, via_send, via_recv, red_send, red_recv, round_sem,
):
    d = lax.axis_index("dp")
    t = lax.axis_index("tensor")
    n_y = n_dp // NX
    n_z = n_tensor // 2
    x, y = lax.rem(d, NX), lax.div(d, NX)
    c, z = lax.rem(t, 2), lax.div(t, 2)
    q = lax.rem(x + c, 2)
    experts = weights.shape[0]
    ff = gate_h.shape[1]

    def peer(dx, dy):
        return lax.rem(y + dy, n_y) * NX + lax.rem(x + dx, NX)

    def source(dx, dy):
        return lax.rem(y + n_y - dy, n_y) * NX + lax.rem(x + NX - dx, NX)

    def z_at(offset):
        return lax.rem(z + offset + n_z, n_z)

    sibling = z * 2 + 1 - c

    def copy_to(src, dst, send, recv_sem, dp=None, tensor=None):
        to = {}
        if dp is not None:
            to["dp"] = dp
        if tensor is not None:
            to["tensor"] = tensor
        return pltpu.make_async_remote_copy(
            src_ref=src, dst_ref=dst, send_sem=send, recv_sem=recv_sem,
            device_id=to, device_id_type=MESH,
        )

    loads = [
        pltpu.make_async_copy(router_h, router, load_sem.at[0]),
        pltpu.make_async_copy(carry_h, carry, load_sem.at[1]),
        pltpu.make_async_copy(tok_h, tok, load_sem.at[2]),
        pltpu.make_async_copy(gate_h, weights.at[:, 0:ff, :], load_sem.at[3]),
        pltpu.make_async_copy(up_h, weights.at[:, ff : 2 * ff, :], load_sem.at[4]),
        pltpu.make_async_copy(down_h, weights.at[:, 2 * ff : 3 * ff, :], load_sem.at[5]),
    ]
    for load in loads:
        load.start()

    barrier = pltpu.get_barrier_semaphore()
    for dx, dy in OFFSETS:
        pl.semaphore_signal(barrier, inc=1, device_id={"dp": peer(dx, dy)}, device_id_type=MESH)
    neighbours = [z_at(1) * 2 + c, z_at(-1) * 2 + c]
    for tensor in [sibling] + neighbours:
        pl.semaphore_signal(barrier, inc=1, device_id={"tensor": tensor}, device_id_type=MESH)

    width = experts * STEP
    spread = lax.broadcasted_iota(jnp.int32, (experts, width), 1) // STEP == lax.broadcasted_iota(
        jnp.int32, (experts, width), 0
    )
    for load in loads[:3]:
        load.wait()
    acc = jnp.zeros((experts, LANES), jnp.float32)
    for i in range(tok.shape[1] // LANES):
        block = tok[:, i * LANES : (i + 1) * LANES].astype(jnp.float32)
        mean = jnp.sum(block, axis=0, keepdims=True) / SEG
        mean = jnp.where(d == n_dp - 1, carry[i : i + 1, :], mean)
        acc += router[:, i * LANES : (i + 1) * LANES] * mean
    total = jnp.sum(acc, axis=1, keepdims=True)
    logits = CAP * jnp.tanh(total / CAP)
    scores = jnp.exp(logits)
    probs = scores / jnp.sum(scores, axis=0, keepdims=True)
    probs = probs.astype(jnp.bfloat16).astype(jnp.float32)
    own_row = jnp.sum(jnp.where(spread, probs, 0.0), axis=0, keepdims=True)
    row_out[...] = own_row
    row_in[d] = own_row

    pl.semaphore_wait(barrier, len(OFFSETS) + 3)

    rows = []
    for j, (dx, dy) in enumerate(OFFSETS):
        rows.append(
            copy_to(row_out, row_in.at[d], row_send.at[j], row_recv.at[d], dp=peer(dx, dy))
        )
        rows[-1].start()
    for load in loads[3:]:
        load.wait()

    diag = lax.rem(lax.broadcasted_iota(jnp.int32, (STEP, width), 1), STEP) == lax.broadcasted_iota(
        jnp.int32, (STEP, width), 0
    )

    def merge(left, first, start):
        count = left.shape[0] // STEP
        right = weights[:, start : start + STEP, :].reshape(width, LANES)
        both = jnp.dot(left, right, preferred_element_type=jnp.float32)
        merged[first : first + count, start : start + STEP, :] = both.astype(jnp.bfloat16).reshape(
            count, STEP, LANES
        )

    gu = []
    lefts = []
    for group in READY:
        left = []
        for dx, dy in group:
            src = lax.rem(peer(dx, dy) + n_dp - 1, n_dp)

            @pl.when(src != d)
            def _():
                copy_to(row_out, row_in.at[src], row_send.at[0], row_recv.at[src], dp=src).wait_recv()

            left.append(jnp.where(diag, row_in[src], 0.0).astype(jnp.bfloat16))
        left = jnp.concatenate(left, axis=0)
        first = ALL.index(group[0])
        lefts.append((left, first))
        for start in range(0, 2 * ff, STEP):
            merge(left, first, start)
        for offset in group:
            if offset == (0, 0):
                continue
            j = OFFSETS.index(offset)
            gu.append(
                copy_to(
                    merged.at[j, 0 : 2 * ff, :], recv.at[j], gu_send.at[j], gu_recv.at[j],
                    dp=peer(*offset),
                )
            )
            gu[-1].start()

    starts = list(range(2 * ff, 3 * ff - STEP + 1, STEP))
    if starts[-1] + STEP < 3 * ff:
        starts.append(3 * ff - STEP)
    for left, first in lefts:
        for start in starts:
            merge(left, first, start)
    own_at = len(OFFSETS)
    half_rows = pl.ds(pl.multiple_of(c * ff, 16), ff)
    dn = {}
    for g, group in enumerate(SLOTS):
        for s, (a, dy) in enumerate(group):
            slot = SLOT_LIST.index((a, dy))
            for dx in (2 * a, 2 * a + 1):
                if (dx, dy) == (0, 0):
                    continue
                j = OFFSETS.index((dx, dy))
                dn[dx, dy] = copy_to(
                    merged.at[j, 2 * ff : 3 * ff, :], recv_dn.at[slot, half_rows, :],
                    dn_send.at[j], dn_recv.at[slot, c],
                    dp=peer(dx, dy), tensor=z * 2 + lax.rem(x, 2),
                )
                dn[dx, dy].start()
    own_copy = copy_to(
        merged.at[own_at, 2 * ff : 3 * ff, :], recv_dn.at[0, half_rows, :],
        own_send, dn_recv.at[0, c], tensor=sibling,
    )

    @pl.when(q == 1)
    def _():
        own_copy.start()

    @pl.when(q == 0)
    def _():
        recv_dn[0, half_rows, :] = merged[own_at, 2 * ff : 3 * ff, :]

    order = [own_at] + list(range(len(OFFSETS)))
    nt = (((1,), (1,)), ((), ()))
    for g in range(0, len(order), 4):
        for tensor in neighbours:
            pl.semaphore_signal(
                round_sem.at[g // 4], inc=1, device_id={"tensor": tensor}, device_id_type=MESH
            )
        left, right_g, right_u = [], [], []
        for j in order[g : g + 4]:
            if j == own_at:
                src, block = d, merged.at[own_at]
            else:
                gu[j].wait_recv()
                src, block = source(*OFFSETS[j]), recv.at[j]
            left.append(tok[:, pl.ds(pl.multiple_of(src * LANES, LANES), LANES)])
            right_g.append(block[0:ff, :])
            right_u.append(block[ff : 2 * ff, :])
        left = jnp.concatenate(left, axis=1)
        more_g = lax.dot_general(
            left, jnp.concatenate(right_g, axis=1), nt, preferred_element_type=jnp.float32
        )
        more_u = lax.dot_general(
            left, jnp.concatenate(right_u, axis=1), nt, preferred_element_type=jnp.float32
        )
        if g == 0:
            acc_g[...] = more_g
            acc_u[...] = more_u
        else:
            acc_g[...] += more_g
            acc_u[...] += more_u
        pl.semaphore_wait(round_sem.at[g // 4], 2)
    gate = acc_g[...]
    hid[c] = (gate / (1.0 + jnp.exp(-gate)) * acc_u[...]).astype(jnp.bfloat16)
    swap = copy_to(hid.at[c], hid.at[c], hid_send, hid_recv, tensor=sibling)
    swap.start()
    swap.wait_recv()

    block = part.shape[1]
    via, red = {}, {}

    def span(g):
        low = sum(len(group) for group in SLOTS[:g]) * LANES
        return slice(low, low + len(SLOTS[g]) * LANES)

    def to_relay(g, n, to, hops):
        rows_at = pl.ds(pl.multiple_of(z_at(to) * 2, 2), 2)
        via[g, n] = copy_to(
            part.at[rows_at, :, span(g)], via_in.at[n, :, :, span(g)],
            via_send.at[g, n], via_recv.at[g, n], tensor=z_at(hops) * 2 + c,
        )
        via[g, n].start()

    def to_owner(g, n, buffer, row, chip, core):
        red[g, n, core] = copy_to(
            buffer.at[row, :, span(g)], red_in.at[n, c, :, span(g)],
            red_send.at[g, n, core], red_recv.at[g, n, c], tensor=z_at(chip) * 2 + core,
        )
        red[g, n, core].start()

    def begin(g):
        for a, dy in SLOTS[g]:
            slot = SLOT_LIST.index((a, dy))
            low = copy_to(
                merged.at[0, 2 * ff : 3 * ff, :], recv_dn.at[slot, 0:ff, :],
                dn_send.at[0], dn_recv.at[slot, 0], tensor=sibling,
            )
            high = copy_to(
                merged.at[0, 2 * ff : 3 * ff, :], recv_dn.at[slot, ff : 2 * ff, :],
                dn_send.at[0], dn_recv.at[slot, 1], tensor=sibling,
            )
            if slot:
                low.wait_recv()
                high.wait_recv()
            else:

                @pl.when((q == 1) | (c == 1))
                def _():
                    low.wait_recv()

                @pl.when((q == 1) | (c == 0))
                def _():
                    high.wait_recv()

        term = None
        for core in range(2):
            right = jnp.concatenate(
                [
                    recv_dn[SLOT_LIST.index(at), core * ff : (core + 1) * ff, :]
                    for at in SLOTS[g]
                ],
                axis=1,
            )
            more = jnp.dot(hid[core], right, preferred_element_type=jnp.float32)
            term = more if term is None else term + more
        part[:, :, span(g)] = term.astype(jnp.bfloat16).reshape(n_tensor, block, -1)
        to_relay(g, 2, 4, 2 - 4 * (g % 2))
        to_relay(g, 0, 3, 1)
        to_relay(g, 1, -3, -1)
        for n, way in ((1, 1), (2, -1)):
            for core in (0, 1):
                to_owner(g, n, part, z_at(way) * 2 + core, way, core)
        red[g, 0, 0] = copy_to(
            part.at[sibling, :, span(g)], red_in.at[0, c, :, span(g)],
            red_send.at[g, 0, 0], red_recv.at[g, 0, c], tensor=sibling,
        )
        red[g, 0, 0].start()

    def relay(g):
        for n in (2, 0, 1):
            via[g, n].wait_recv()
        for n, way in ((0, 1), (1, -1)):
            rows_at = pl.ds(pl.multiple_of(z_at(2 * way) * 2, 2), 2)
            value = part[rows_at, :, span(g)].astype(jnp.float32)
            value = value + via_in[n, :, :, span(g)].astype(jnp.float32)
            if n == g % 2:
                value = value + via_in[2, :, :, span(g)].astype(jnp.float32)
            via_out[n, :, :, span(g)] = value.astype(jnp.bfloat16)
            for core in (0, 1):
                to_owner(g, 3 + n, via_out.at[n], core, 2 * way, core)

    def finish(g):
        for n in range(5):
            for core in (c, 1 - c) if n else (1 - c,):
                copy_to(
                    part.at[t, :, span(g)], red_in.at[n, core, :, span(g)],
                    red_send.at[g, 0, 0], red_recv.at[g, n, core], tensor=sibling,
                ).wait_recv()
        for of in range(2):
            core = c if of == 0 else 1 - c
            value = (part[t, :, span(g)] if of == 0 else red_in[0, core, :, span(g)]).astype(
                jnp.float32
            )
            for n in range(1, 5):
                value = value + red_in[n, core, :, span(g)].astype(jnp.float32)
            odd = lax.rem(x + core, 2)
            for s, (a, dy) in enumerate(SLOTS[g]):
                src = source(2 * a + odd, dy)
                out_ref[:, pl.ds(pl.multiple_of(src * LANES, LANES), LANES)] = value[
                    :, s * LANES : (s + 1) * LANES
                ].astype(jnp.bfloat16)

    n_groups = len(SLOTS)
    for g in range(n_groups):
        begin(g)
        if g:
            relay(g - 1)
    relay(n_groups - 1)
    for g in range(n_groups):
        finish(g)

    for copy in rows + gu + list(dn.values()):
        copy.wait_send()

    @pl.when(q == 1)
    def _():
        own_copy.wait_send()

    swap.wait_send()
    for copy in list(via.values()) + list(red.values()):
        copy.wait_send()


def solution(mesh):
    n_dp, n_tensor = mesh.shape["dp"], mesh.shape["tensor"]

    def on_device(tokens, gate_weight, up_weight, down_weight, router_weight, carry_mean):
        rows, width = tokens.shape
        experts, _, ff = gate_weight.shape
        n_z = n_tensor // 2
        peers = len(OFFSETS)
        groups = len(SLOTS)
        block = rows // n_tensor
        cols = len(SLOT_LIST) * LANES
        bf16, f32 = jnp.bfloat16, jnp.float32
        dma = pltpu.SemaphoreType.DMA
        return pl.pallas_call(
            functools.partial(kernel, n_dp, n_tensor),
            out_shape=jax.ShapeDtypeStruct((block, width), bf16),
            in_specs=[pl.BlockSpec(memory_space=pltpu.HBM)] * 6,
            out_specs=pl.BlockSpec(memory_space=pltpu.VMEM),
            scratch_shapes=[
                pltpu.VMEM((rows, width), bf16),
                pltpu.VMEM((experts, 3 * ff, LANES), bf16),
                pltpu.VMEM((experts, width), f32),
                pltpu.VMEM((width // LANES, LANES), f32),
                pltpu.VMEM((1, experts * STEP), f32),
                pltpu.VMEM((n_dp, 1, experts * STEP), f32),
                pltpu.VMEM((n_dp, 3 * ff, LANES), bf16),
                pltpu.VMEM((peers, 2 * ff, LANES), bf16),
                pltpu.VMEM((n_dp // 2, 2 * ff, LANES), bf16),
                pltpu.VMEM((rows, ff), f32),
                pltpu.VMEM((rows, ff), f32),
                pltpu.VMEM((2, rows, ff), bf16),
                pltpu.VMEM((n_tensor, block, cols), bf16),
                pltpu.VMEM((3, 2, block, cols), bf16),
                pltpu.VMEM((2, 2, block, cols), bf16),
                pltpu.VMEM((5, 2, block, cols), bf16),
                dma((6,)),
                dma((peers,)), dma((n_dp,)),
                dma((peers,)), dma((peers,)),
                dma((peers,)), dma((n_dp // 2, 2)), dma(()),
                dma(()), dma(()),
                dma((groups, 3)), dma((groups, 3)),
                dma((groups, 5, 2)), dma((groups, 5, 2)),
                pltpu.SemaphoreType.REGULAR((4,)),
            ],
            compiler_params=pltpu.CompilerParams(
                collective_id=0, has_side_effects=True, vmem_limit_bytes=32 << 20
            ),
        )(
            *(
                pltpu.with_memory_space_constraint(operand, pltpu.HBM)
                for operand in (
                    tokens,
                    jnp.transpose(gate_weight, (0, 2, 1)),
                    jnp.transpose(up_weight, (0, 2, 1)),
                    down_weight,
                    router_weight.T,
                    carry_mean.reshape(width // LANES, LANES),
                )
            )
        )

    placed = (
        P("dp", None),
        P(None, "dp", "tensor"),
        P(None, "dp", "tensor"),
        P(None, "tensor", "dp"),
        P(),
        P(),
    )
    return jax.shard_map(
        on_device, mesh=mesh, in_specs=placed, out_specs=P(("dp", "tensor"), None), check_vma=False
    )
```

```python
import functools

import jax
import jax.numpy as jnp
from jax import lax
from jax.experimental import pallas as pl
from jax.experimental.pallas import tpu as pltpu
from jax.sharding import PartitionSpec as P

MESH = pl.DeviceIdType.MESH
SEG = 256
CAP = 8.0
NX = 4
LANES = 128
STEP = 32

READY = (
    ((2, 2), (2, 1), (2, 3), (1, 2), (3, 2), (2, 0), (0, 2), (1, 1)),
    ((3, 3), (1, 3), (3, 1), (1, 0), (3, 0), (0, 1), (0, 3), (0, 0)),
)
OFFSETS = tuple(o for group in READY for o in group if o != (0, 0))
ALL = OFFSETS + ((0, 0),)
SLOTS = (((0, 0), (1, 2), (0, 2), (1, 0)), ((0, 1), (1, 3), (0, 3), (1, 1)))


def kernel(
    n_dp, n_tensor,
    tok_h, gate_h, up_h, down_h, router_h, carry_h, out_ref,
    tok, weights, router, carry, row_out, row_in, merged, recv, recv_dn,
    acc_g, acc_u, hid, part, via_in, via_out, red_in,
    load_sem, row_send, row_recv, gu_send, gu_recv, dn_send, dn_recv, own_send, own_recv,
    hid_send, hid_recv, via_send, via_recv, red_send, red_recv, round_sem,
):
    d = lax.axis_index("dp")
    t = lax.axis_index("tensor")
    n_y = n_dp // NX
    n_z = n_tensor // 2
    x, y = lax.rem(d, NX), lax.div(d, NX)
    c, z = lax.rem(t, 2), lax.div(t, 2)
    q = lax.rem(x + c, 2)
    experts = weights.shape[0]
    ff = gate_h.shape[1]

    def peer(dx, dy):
        return lax.rem(y + dy, n_y) * NX + lax.rem(x + dx, NX)

    def source(dx, dy):
        return lax.rem(y + n_y - dy, n_y) * NX + lax.rem(x + NX - dx, NX)

    def z_at(offset):
        return lax.rem(z + offset + n_z, n_z)

    sibling = z * 2 + 1 - c

    def copy_to(src, dst, send, recv_sem, dp=None, tensor=None):
        to = {}
        if dp is not None:
            to["dp"] = dp
        if tensor is not None:
            to["tensor"] = tensor
        return pltpu.make_async_remote_copy(
            src_ref=src, dst_ref=dst, send_sem=send, recv_sem=recv_sem,
            device_id=to, device_id_type=MESH,
        )

    def wait_all(ref, sem):
        pltpu.make_async_copy(ref, ref, sem).wait()

    loads = [
        pltpu.make_async_copy(router_h, router, load_sem.at[0]),
        pltpu.make_async_copy(carry_h, carry, load_sem.at[1]),
        pltpu.make_async_copy(tok_h, tok, load_sem.at[2]),
        pltpu.make_async_copy(gate_h, weights.at[:, 0:ff, :], load_sem.at[3]),
        pltpu.make_async_copy(up_h, weights.at[:, ff : 2 * ff, :], load_sem.at[3]),
        pltpu.make_async_copy(down_h, weights.at[:, 2 * ff : 3 * ff, :], load_sem.at[3]),
    ]
    for load in loads:
        load.start()

    barrier = pltpu.get_barrier_semaphore()
    for dx, dy in OFFSETS:
        pl.semaphore_signal(barrier, inc=1, device_id={"dp": peer(dx, dy)}, device_id_type=MESH)
    neighbours = [z_at(1) * 2 + c, z_at(-1) * 2 + c]
    for tensor in [sibling] + neighbours:
        pl.semaphore_signal(barrier, inc=1, device_id={"tensor": tensor}, device_id_type=MESH)

    width = experts * STEP
    spread = lax.broadcasted_iota(jnp.int32, (experts, width), 1) // STEP == lax.broadcasted_iota(
        jnp.int32, (experts, width), 0
    )
    for load in loads[:3]:
        load.wait()
    acc = jnp.zeros((experts, LANES), jnp.float32)
    for i in range(tok.shape[1] // LANES):
        block = tok[:, i * LANES : (i + 1) * LANES].astype(jnp.float32)
        mean = jnp.sum(block, axis=0, keepdims=True) / SEG
        mean = jnp.where(d == n_dp - 1, carry[i : i + 1, :], mean)
        acc += router[:, i * LANES : (i + 1) * LANES] * mean
    total = jnp.sum(acc, axis=1, keepdims=True)
    logits = CAP * jnp.tanh(total / CAP)
    scores = jnp.exp(logits)
    probs = scores / jnp.sum(scores, axis=0, keepdims=True)
    probs = probs.astype(jnp.bfloat16).astype(jnp.float32)
    own_row = jnp.sum(jnp.where(spread, probs, 0.0), axis=0, keepdims=True)
    row_out[...] = own_row
    row_in[d] = own_row

    pl.semaphore_wait(barrier, len(OFFSETS) + 3)

    for dx, dy in OFFSETS:
        copy_to(row_out, row_in.at[d], row_send, row_recv, dp=peer(dx, dy)).start()
    wait_all(weights, load_sem.at[3])
    wait_all(row_in.at[0 : len(OFFSETS)], row_recv)

    diag = lax.rem(lax.broadcasted_iota(jnp.int32, (STEP, width), 1), STEP) == lax.broadcasted_iota(
        jnp.int32, (STEP, width), 0
    )

    def merge(left, first, start):
        count = left.shape[0] // STEP
        right = weights[:, start : start + STEP, :].reshape(width, LANES)
        both = jnp.dot(left, right, preferred_element_type=jnp.float32)
        merged[first : first + count, start : start + STEP, :] = both.astype(jnp.bfloat16).reshape(
            count, STEP, LANES
        )

    lefts = []
    for group in READY:
        left = []
        for dx, dy in group:
            src = lax.rem(peer(dx, dy) + n_dp - 1, n_dp)
            left.append(jnp.where(diag, row_in[src], 0.0).astype(jnp.bfloat16))
        left = jnp.concatenate(left, axis=0)
        first = ALL.index(group[0])
        lefts.append((left, first))
        for start in range(0, 2 * ff, STEP):
            merge(left, first, start)
        for offset in group:
            if offset == (0, 0):
                continue
            j = OFFSETS.index(offset)
            copy_to(
                merged.at[j, 0 : 2 * ff, :], recv.at[j], gu_send, gu_recv.at[(j + 1) // 4],
                dp=peer(*offset),
            ).start()

    starts = list(range(2 * ff, 3 * ff - STEP + 1, STEP))
    if starts[-1] + STEP < 3 * ff:
        starts.append(3 * ff - STEP)
    for left, first in lefts:
        for start in starts:
            merge(left, first, start)
    own_at = len(OFFSETS)
    half_rows = pl.ds(pl.multiple_of(c * ff, 16), ff)
    for g, group in enumerate(SLOTS):
        for s, (a, dy) in enumerate(group):
            for dx in (2 * a, 2 * a + 1):
                if (dx, dy) == (0, 0):
                    continue
                copy_to(
                    merged.at[OFFSETS.index((dx, dy)), 2 * ff : 3 * ff, :],
                    recv_dn.at[g, s, half_rows, :],
                    dn_send, dn_recv.at[g],
                    dp=peer(dx, dy), tensor=z * 2 + lax.rem(x, 2),
                ).start()
    own_copy = copy_to(
        merged.at[own_at, 2 * ff : 3 * ff, :], recv_dn.at[0, 0, half_rows, :],
        own_send, own_recv, tensor=sibling,
    )

    @pl.when(q == 1)
    def _():
        own_copy.start()

    @pl.when(q == 0)
    def _():
        recv_dn[0, 0, half_rows, :] = merged[own_at, 2 * ff : 3 * ff, :]

    order = [own_at] + list(range(len(OFFSETS)))
    nt = (((1,), (1,)), ((), ()))
    for g in range(0, len(order), 4):
        first, last = max(g, 1) - 1, min(g + 3, len(OFFSETS))
        if g // 4 < 2:
            for tensor in neighbours:
                pl.semaphore_signal(
                    round_sem.at[g // 4], inc=1, device_id={"tensor": tensor}, device_id_type=MESH
                )
        wait_all(recv.at[first:last], gu_recv.at[g // 4])
        left, right_g, right_u = [], [], []
        for j in order[g : g + 4]:
            if j == own_at:
                src, block = d, merged.at[own_at]
            else:
                src, block = source(*OFFSETS[j]), recv.at[j]
            left.append(tok[:, pl.ds(pl.multiple_of(src * LANES, LANES), LANES)])
            right_g.append(block[0:ff, :])
            right_u.append(block[ff : 2 * ff, :])
        left = jnp.concatenate(left, axis=1)
        more_g = lax.dot_general(
            left, jnp.concatenate(right_g, axis=1), nt, preferred_element_type=jnp.float32
        )
        more_u = lax.dot_general(
            left, jnp.concatenate(right_u, axis=1), nt, preferred_element_type=jnp.float32
        )
        if g == 0:
            acc_g[...] = more_g
            acc_u[...] = more_u
        else:
            acc_g[...] += more_g
            acc_u[...] += more_u
        if g // 4 < 2:
            pl.semaphore_wait(round_sem.at[g // 4], 2)
    gate = acc_g[...]
    hid[c] = (gate / (1.0 + jnp.exp(-gate)) * acc_u[...]).astype(jnp.bfloat16)
    swap = copy_to(hid.at[c], hid.at[c], hid_send, hid_recv, tensor=sibling)
    swap.start()
    swap.wait_recv()

    block = part.shape[2]

    def to_owner(g, n, buffer, row, chip, core):
        copy_to(
            buffer.at[row], red_in.at[g, 2 * n + c], red_send, red_recv.at[g],
            tensor=z_at(chip) * 2 + core,
        ).start()

    def begin(g):
        if g == 0:

            @pl.when(q == 0)
            def _():
                wait_all(recv_dn.at[0, 0, half_rows, :], own_recv)
                wait_all(recv_dn.at[0, 1:], dn_recv.at[0])

            @pl.when(q == 1)
            def _():
                wait_all(recv_dn.at[0], dn_recv.at[0])

        else:
            wait_all(recv_dn.at[g], dn_recv.at[g])
        term = None
        for core in range(2):
            right = jnp.concatenate(
                [recv_dn[g, s, core * ff : (core + 1) * ff, :] for s in range(len(SLOTS[g]))], axis=1
            )
            more = jnp.dot(hid[core], right, preferred_element_type=jnp.float32)
            term = more if term is None else term + more
        part[g] = term.astype(jnp.bfloat16).reshape(n_tensor, block, -1)
        for n, owner, hops in ((2, 4, 2 - 4 * g), (0, 3, 1), (1, -3, -1)):
            rows_at = pl.ds(pl.multiple_of(z_at(owner) * 2, 2), 2)
            copy_to(
                part.at[g, rows_at], via_in.at[g, n], via_send, via_recv.at[g],
                tensor=z_at(hops) * 2 + c,
            ).start()
        for n, way in ((0, 1), (1, -1)):
            for core in (0, 1):
                to_owner(g, n, part.at[g], z_at(way) * 2 + core, way, core)
        copy_to(
            part.at[g, sibling], red_in.at[g, 8], red_send, red_recv.at[g], tensor=sibling
        ).start()

    def relay(g):
        wait_all(via_in.at[g], via_recv.at[g])
        for n, way in ((0, 1), (1, -1)):
            rows_at = pl.ds(pl.multiple_of(z_at(2 * way) * 2, 2), 2)
            value = part[g, rows_at].astype(jnp.float32) + via_in[g, n].astype(jnp.float32)
            if n == g:
                value = value + via_in[g, 2].astype(jnp.float32)
            via_out[g, n] = value.astype(jnp.bfloat16)
            for core in (0, 1):
                to_owner(g, 2 + n, via_out.at[g, n], core, 2 * way, core)

    def finish(g):
        wait_all(red_in.at[g], red_recv.at[g])
        for of in range(2):
            core = c if of == 0 else 1 - c
            value = (part[g, t] if of == 0 else red_in[g, 8]).astype(jnp.float32)
            for n in range(4):
                value = value + red_in[g, 2 * n + core].astype(jnp.float32)
            odd = lax.rem(x + core, 2)
            for s, (a, dy) in enumerate(SLOTS[g]):
                src = source(2 * a + odd, dy)
                out_ref[:, pl.ds(pl.multiple_of(src * LANES, LANES), LANES)] = value[
                    :, s * LANES : (s + 1) * LANES
                ].astype(jnp.bfloat16)

    n_groups = len(SLOTS)
    for g in range(n_groups):
        begin(g)
    for g in range(n_groups):
        relay(g)
    for g in range(n_groups):
        finish(g)

    peers = len(OFFSETS)
    wait_all(row_in.at[0:peers], row_send)
    wait_all(merged.at[0:peers, 0 : 2 * ff, :], gu_send)
    wait_all(merged.at[0:peers, 2 * ff : 3 * ff, :], dn_send)
    wait_all(via_in, via_send)
    wait_all(red_in, red_send)

    @pl.when(q == 1)
    def _():
        own_copy.wait_send()

    swap.wait_send()


def solution(mesh):
    n_dp, n_tensor = mesh.shape["dp"], mesh.shape["tensor"]

    def on_device(tokens, gate_weight, up_weight, down_weight, router_weight, carry_mean):
        rows, width = tokens.shape
        experts, _, ff = gate_weight.shape
        peers = len(OFFSETS)
        groups = len(SLOTS)
        block = rows // n_tensor
        slots = len(SLOTS[0])
        cols = slots * LANES
        bf16, f32 = jnp.bfloat16, jnp.float32
        dma = pltpu.SemaphoreType.DMA
        return pl.pallas_call(
            functools.partial(kernel, n_dp, n_tensor),
            out_shape=jax.ShapeDtypeStruct((block, width), bf16),
            in_specs=[pl.BlockSpec(memory_space=pltpu.HBM)] * 6,
            out_specs=pl.BlockSpec(memory_space=pltpu.VMEM),
            scratch_shapes=[
                pltpu.VMEM((rows, width), bf16),
                pltpu.VMEM((experts, 3 * ff, LANES), bf16),
                pltpu.VMEM((experts, width), f32),
                pltpu.VMEM((width // LANES, LANES), f32),
                pltpu.VMEM((1, experts * STEP), f32),
                pltpu.VMEM((n_dp, 1, experts * STEP), f32),
                pltpu.VMEM((n_dp, 3 * ff, LANES), bf16),
                pltpu.VMEM((peers, 2 * ff, LANES), bf16),
                pltpu.VMEM((groups, slots, 2 * ff, LANES), bf16),
                pltpu.VMEM((rows, ff), f32),
                pltpu.VMEM((rows, ff), f32),
                pltpu.VMEM((2, rows, ff), bf16),
                pltpu.VMEM((groups, n_tensor, block, cols), bf16),
                pltpu.VMEM((groups, 3, 2, block, cols), bf16),
                pltpu.VMEM((groups, 2, 2, block, cols), bf16),
                pltpu.VMEM((groups, 9, block, cols), bf16),
                dma((4,)),
                dma(()), dma(()),
                dma(()), dma((4,)),
                dma(()), dma((groups,)), dma(()), dma(()),
                dma(()), dma(()),
                dma(()), dma((groups,)),
                dma(()), dma((groups,)),
                pltpu.SemaphoreType.REGULAR((2,)),
            ],
            compiler_params=pltpu.CompilerParams(
                collective_id=0, has_side_effects=True, vmem_limit_bytes=32 << 20
            ),
        )(
            *(
                pltpu.with_memory_space_constraint(operand, pltpu.HBM)
                for operand in (
                    tokens,
                    jnp.transpose(gate_weight, (0, 2, 1)),
                    jnp.transpose(up_weight, (0, 2, 1)),
                    down_weight,
                    router_weight.T,
                    carry_mean.reshape(width // LANES, LANES),
                )
            )
        )

    placed = (
        P("dp", None),
        P(None, "dp", "tensor"),
        P(None, "dp", "tensor"),
        P(None, "tensor", "dp"),
        P(),
        P(),
    )
    return jax.shard_map(
        on_device, mesh=mesh, in_specs=placed, out_specs=P(("dp", "tensor"), None), check_vma=False
    )
```

```python
import functools

import jax
import jax.numpy as jnp
from jax import lax
from jax.experimental import pallas as pl
from jax.experimental.pallas import tpu as pltpu
from jax.sharding import PartitionSpec as P

MESH = pl.DeviceIdType.MESH
SEG = 256
CAP = 8.0
NX = 4
LANES = 128
STEP = 32

READY = (
    ((2, 2), (2, 1), (2, 3), (1, 2), (3, 2), (2, 0), (0, 2), (1, 1)),
    ((3, 3), (1, 3), (3, 1), (1, 0), (3, 0), (0, 1), (0, 3), (0, 0)),
)
OFFSETS = tuple(o for group in READY for o in group if o != (0, 0))
ALL = OFFSETS + ((0, 0),)
SLOTS = (((0, 0), (1, 2), (0, 2), (1, 0)), ((0, 1), (1, 3), (0, 3)), ((1, 1),))
DIRECT = (2,)
FIRST = tuple(sum(len(group) for group in SLOTS[:g]) for g in range(len(SLOTS) + 1))


def kernel(
    n_dp, n_tensor,
    tok_h, gate_h, up_h, down_h, router_h, carry_h, out_ref,
    tok, weights, router, carry, row_out, row_in, merged, recv, recv_dn,
    acc_g, acc_u, hid, part, via_in, via_out, red_in,
    load_sem, row_send, row_recv, gu_send, gu_recv, dn_send, dn_recv, own_send, own_recv,
    hid_send, hid_recv, via_send, via_recv, red_send, red_recv, round_sem,
):
    d = lax.axis_index("dp")
    t = lax.axis_index("tensor")
    n_y = n_dp // NX
    n_z = n_tensor // 2
    x, y = lax.rem(d, NX), lax.div(d, NX)
    c, z = lax.rem(t, 2), lax.div(t, 2)
    q = lax.rem(x + c, 2)
    experts = weights.shape[0]
    ff = gate_h.shape[1]

    def peer(dx, dy):
        return lax.rem(y + dy, n_y) * NX + lax.rem(x + dx, NX)

    def source(dx, dy):
        return lax.rem(y + n_y - dy, n_y) * NX + lax.rem(x + NX - dx, NX)

    def z_at(offset):
        return lax.rem(z + offset + n_z, n_z)

    sibling = z * 2 + 1 - c

    def copy_to(src, dst, send, recv_sem, dp=None, tensor=None):
        to = {}
        if dp is not None:
            to["dp"] = dp
        if tensor is not None:
            to["tensor"] = tensor
        return pltpu.make_async_remote_copy(
            src_ref=src, dst_ref=dst, send_sem=send, recv_sem=recv_sem,
            device_id=to, device_id_type=MESH,
        )

    def wait_all(ref, sem):
        pltpu.make_async_copy(ref, ref, sem).wait()

    loads = [
        pltpu.make_async_copy(router_h, router, load_sem.at[0]),
        pltpu.make_async_copy(carry_h, carry, load_sem.at[1]),
        pltpu.make_async_copy(tok_h, tok, load_sem.at[2]),
        pltpu.make_async_copy(gate_h, weights.at[:, 0:ff, :], load_sem.at[3]),
        pltpu.make_async_copy(up_h, weights.at[:, ff : 2 * ff, :], load_sem.at[3]),
        pltpu.make_async_copy(down_h, weights.at[:, 2 * ff : 3 * ff, :], load_sem.at[3]),
    ]
    for load in loads:
        load.start()

    barrier = pltpu.get_barrier_semaphore()
    for dx, dy in OFFSETS:
        pl.semaphore_signal(barrier, inc=1, device_id={"dp": peer(dx, dy)}, device_id_type=MESH)
    neighbours = [z_at(1) * 2 + c, z_at(-1) * 2 + c]
    for tensor in [sibling] + neighbours:
        pl.semaphore_signal(barrier, inc=1, device_id={"tensor": tensor}, device_id_type=MESH)

    width = experts * STEP
    spread = lax.broadcasted_iota(jnp.int32, (experts, width), 1) // STEP == lax.broadcasted_iota(
        jnp.int32, (experts, width), 0
    )
    for load in loads[:3]:
        load.wait()
    acc = jnp.zeros((experts, LANES), jnp.float32)
    for i in range(tok.shape[1] // LANES):
        block = tok[:, i * LANES : (i + 1) * LANES].astype(jnp.float32)
        mean = jnp.sum(block, axis=0, keepdims=True) / SEG
        mean = jnp.where(d == n_dp - 1, carry[i : i + 1, :], mean)
        acc += router[:, i * LANES : (i + 1) * LANES] * mean
    total = jnp.sum(acc, axis=1, keepdims=True)
    logits = CAP * jnp.tanh(total / CAP)
    scores = jnp.exp(logits)
    probs = scores / jnp.sum(scores, axis=0, keepdims=True)
    probs = probs.astype(jnp.bfloat16).astype(jnp.float32)
    own_row = jnp.sum(jnp.where(spread, probs, 0.0), axis=0, keepdims=True)
    row_out[...] = own_row
    row_in[d] = own_row

    pl.semaphore_wait(barrier, len(OFFSETS) + 3)

    for dx, dy in OFFSETS:
        copy_to(row_out, row_in.at[d], row_send, row_recv, dp=peer(dx, dy)).start()
    wait_all(weights, load_sem.at[3])
    wait_all(row_in.at[0 : len(OFFSETS)], row_recv)

    diag = lax.rem(lax.broadcasted_iota(jnp.int32, (STEP, width), 1), STEP) == lax.broadcasted_iota(
        jnp.int32, (STEP, width), 0
    )

    def merge(left, first, start):
        count = left.shape[0] // STEP
        right = weights[:, start : start + STEP, :].reshape(width, LANES)
        both = jnp.dot(left, right, preferred_element_type=jnp.float32)
        merged[first : first + count, start : start + STEP, :] = both.astype(jnp.bfloat16).reshape(
            count, STEP, LANES
        )

    lefts = []
    for group in READY:
        left = []
        for dx, dy in group:
            src = lax.rem(peer(dx, dy) + n_dp - 1, n_dp)
            left.append(jnp.where(diag, row_in[src], 0.0).astype(jnp.bfloat16))
        left = jnp.concatenate(left, axis=0)
        first = ALL.index(group[0])
        lefts.append((left, first))
        for start in range(0, 2 * ff, STEP):
            merge(left, first, start)
        for offset in group:
            if offset == (0, 0):
                continue
            j = OFFSETS.index(offset)
            copy_to(
                merged.at[j, 0 : 2 * ff, :], recv.at[j], gu_send, gu_recv.at[(j + 1) // 4],
                dp=peer(*offset),
            ).start()

    starts = list(range(2 * ff, 3 * ff - STEP + 1, STEP))
    if starts[-1] + STEP < 3 * ff:
        starts.append(3 * ff - STEP)
    for left, first in lefts:
        for start in starts:
            merge(left, first, start)
    own_at = len(OFFSETS)
    half_rows = pl.ds(pl.multiple_of(c * ff, 16), ff)
    for g, group in enumerate(SLOTS):
        for s, (a, dy) in enumerate(group):
            for dx in (2 * a, 2 * a + 1):
                if (dx, dy) == (0, 0):
                    continue
                copy_to(
                    merged.at[OFFSETS.index((dx, dy)), 2 * ff : 3 * ff, :],
                    recv_dn.at[FIRST[g] + s, half_rows, :],
                    dn_send, dn_recv.at[g],
                    dp=peer(dx, dy), tensor=z * 2 + lax.rem(x, 2),
                ).start()
    own_copy = copy_to(
        merged.at[own_at, 2 * ff : 3 * ff, :], recv_dn.at[0, half_rows, :],
        own_send, own_recv, tensor=sibling,
    )

    @pl.when(q == 1)
    def _():
        own_copy.start()

    @pl.when(q == 0)
    def _():
        recv_dn[0, half_rows, :] = merged[own_at, 2 * ff : 3 * ff, :]

    order = [own_at] + list(range(len(OFFSETS)))
    nt = (((1,), (1,)), ((), ()))
    for g in range(0, len(order), 4):
        first, last = max(g, 1) - 1, min(g + 3, len(OFFSETS))
        for tensor in neighbours:
            pl.semaphore_signal(
                round_sem.at[g // 4], inc=1, device_id={"tensor": tensor}, device_id_type=MESH
            )
        wait_all(recv.at[first:last], gu_recv.at[g // 4])
        left, right_g, right_u = [], [], []
        for j in order[g : g + 4]:
            if j == own_at:
                src, block = d, merged.at[own_at]
            else:
                src, block = source(*OFFSETS[j]), recv.at[j]
            left.append(tok[:, pl.ds(pl.multiple_of(src * LANES, LANES), LANES)])
            right_g.append(block[0:ff, :])
            right_u.append(block[ff : 2 * ff, :])
        left = jnp.concatenate(left, axis=1)
        more_g = lax.dot_general(
            left, jnp.concatenate(right_g, axis=1), nt, preferred_element_type=jnp.float32
        )
        more_u = lax.dot_general(
            left, jnp.concatenate(right_u, axis=1), nt, preferred_element_type=jnp.float32
        )
        if g == 0:
            acc_g[...] = more_g
            acc_u[...] = more_u
        else:
            acc_g[...] += more_g
            acc_u[...] += more_u
        pl.semaphore_wait(round_sem.at[g // 4], 2)
    gate = acc_g[...]
    hid[c] = (gate / (1.0 + jnp.exp(-gate)) * acc_u[...]).astype(jnp.bfloat16)
    swap = copy_to(hid.at[c], hid.at[c], hid_send, hid_recv, tensor=sibling)
    swap.start()
    swap.wait_recv()

    block = part.shape[1]
    n_groups = len(SLOTS)
    spans = [slice(FIRST[g] * LANES, FIRST[g + 1] * LANES) for g in range(n_groups)]
    places = [2 * n_z - 2 if g in DIRECT else 8 for g in range(n_groups)]

    def to_owner(g, n, buffer, row, chip, core):
        copy_to(
            buffer.at[row, :, spans[g]], red_in.at[1 + 2 * n + c, :, spans[g]],
            red_send.at[g], red_recv.at[g],
            tensor=z_at(chip) * 2 + core,
        ).start()

    def begin(g):
        if g == 0:

            @pl.when(q == 0)
            def _():
                wait_all(recv_dn.at[0, half_rows, :], own_recv)
                wait_all(recv_dn.at[1 : FIRST[1]], dn_recv.at[0])

            @pl.when(q == 1)
            def _():
                wait_all(recv_dn.at[0 : FIRST[1]], dn_recv.at[0])

        else:
            wait_all(recv_dn.at[FIRST[g] : FIRST[g + 1]], dn_recv.at[g])
        term = None
        for core in range(2):
            right = jnp.concatenate(
                [recv_dn[s, core * ff : (core + 1) * ff, :] for s in range(FIRST[g], FIRST[g + 1])],
                axis=1,
            )
            more = jnp.dot(hid[core], right, preferred_element_type=jnp.float32)
            term = more if term is None else term + more
        part[:, :, spans[g]] = term.astype(jnp.bfloat16).reshape(n_tensor, block, -1)
        if g in DIRECT:
            ways = (4, 3, -3, 2, -2, 1, -1)
        else:
            for n, owner, hops in ((2, 4, 2 - 4 * (g % 2)), (0, 3, 1), (1, -3, -1)):
                rows_at = pl.ds(pl.multiple_of(z_at(owner) * 2, 2), 2)
                copy_to(
                    part.at[rows_at, :, spans[g]], via_in.at[n, :, :, spans[g]],
                    via_send.at[g], via_recv.at[g], tensor=z_at(hops) * 2 + c,
                ).start()
            ways = (1, -1)
        for n, way in enumerate(ways):
            for core in (0, 1):
                to_owner(g, n, part, z_at(way) * 2 + core, way, core)
        copy_to(
            part.at[sibling, :, spans[g]], red_in.at[0, :, spans[g]],
            red_send.at[g], red_recv.at[g], tensor=sibling,
        ).start()

    def relay(g):
        wait_all(via_in.at[:, :, :, spans[g]], via_recv.at[g])
        for n, way in ((0, 1), (1, -1)):
            rows_at = pl.ds(pl.multiple_of(z_at(2 * way) * 2, 2), 2)
            value = part[rows_at, :, spans[g]].astype(jnp.float32)
            value = value + via_in[n, :, :, spans[g]].astype(jnp.float32)
            if n == g % 2:
                value = value + via_in[2, :, :, spans[g]].astype(jnp.float32)
            via_out[n, :, :, spans[g]] = value.astype(jnp.bfloat16)
            for core in (0, 1):
                to_owner(g, 2 + n, via_out.at[n], core, 2 * way, core)

    def finish(g):
        wait_all(red_in.at[0 : 1 + places[g], :, spans[g]], red_recv.at[g])
        for of in range(2):
            core = c if of == 0 else 1 - c
            value = part[t, :, spans[g]] if of == 0 else red_in[0, :, spans[g]]
            value = value.astype(jnp.float32)
            for n in range(places[g] // 2):
                value = value + red_in[1 + 2 * n + core, :, spans[g]].astype(jnp.float32)
            odd = lax.rem(x + core, 2)
            for s, (a, dy) in enumerate(SLOTS[g]):
                src = source(2 * a + odd, dy)
                out_ref[:, pl.ds(pl.multiple_of(src * LANES, LANES), LANES)] = value[
                    :, s * LANES : (s + 1) * LANES
                ].astype(jnp.bfloat16)

    for g in range(n_groups):
        begin(g)
    for g in range(n_groups):
        if g not in DIRECT:
            relay(g)
    for g in range(n_groups):
        finish(g)

    peers = len(OFFSETS)
    wait_all(row_in.at[0:peers], row_send)
    wait_all(merged.at[0:peers, 0 : 2 * ff, :], gu_send)
    wait_all(merged.at[0:peers, 2 * ff : 3 * ff, :], dn_send)
    for g in range(n_groups):
        if g not in DIRECT:
            wait_all(via_in.at[:, :, :, spans[g]], via_send.at[g])
        wait_all(red_in.at[0 : 1 + places[g], :, spans[g]], red_send.at[g])

    @pl.when(q == 1)
    def _():
        own_copy.wait_send()

    swap.wait_send()


def solution(mesh):
    n_dp, n_tensor = mesh.shape["dp"], mesh.shape["tensor"]

    def on_device(tokens, gate_weight, up_weight, down_weight, router_weight, carry_mean):
        rows, width = tokens.shape
        experts, _, ff = gate_weight.shape
        peers = len(OFFSETS)
        groups = len(SLOTS)
        block = rows // n_tensor
        slots = FIRST[-1]
        cols = slots * LANES
        bf16, f32 = jnp.bfloat16, jnp.float32
        dma = pltpu.SemaphoreType.DMA
        return pl.pallas_call(
            functools.partial(kernel, n_dp, n_tensor),
            out_shape=jax.ShapeDtypeStruct((block, width), bf16),
            in_specs=[pl.BlockSpec(memory_space=pltpu.HBM)] * 6,
            out_specs=pl.BlockSpec(memory_space=pltpu.VMEM),
            scratch_shapes=[
                pltpu.VMEM((rows, width), bf16),
                pltpu.VMEM((experts, 3 * ff, LANES), bf16),
                pltpu.VMEM((experts, width), f32),
                pltpu.VMEM((width // LANES, LANES), f32),
                pltpu.VMEM((1, experts * STEP), f32),
                pltpu.VMEM((n_dp, 1, experts * STEP), f32),
                pltpu.VMEM((n_dp, 3 * ff, LANES), bf16),
                pltpu.VMEM((peers, 2 * ff, LANES), bf16),
                pltpu.VMEM((slots, 2 * ff, LANES), bf16),
                pltpu.VMEM((rows, ff), f32),
                pltpu.VMEM((rows, ff), f32),
                pltpu.VMEM((2, rows, ff), bf16),
                pltpu.VMEM((n_tensor, block, cols), bf16),
                pltpu.VMEM((3, 2, block, cols), bf16),
                pltpu.VMEM((2, 2, block, cols), bf16),
                pltpu.VMEM((n_tensor - 1, block, cols), bf16),
                dma((4,)),
                dma(()), dma(()),
                dma(()), dma((4,)),
                dma(()), dma((groups,)), dma(()), dma(()),
                dma(()), dma(()),
                dma((groups,)), dma((groups,)),
                dma((groups,)), dma((groups,)),
                pltpu.SemaphoreType.REGULAR((4,)),
            ],
            compiler_params=pltpu.CompilerParams(
                collective_id=0, has_side_effects=True, vmem_limit_bytes=32 << 20
            ),
        )(
            *(
                pltpu.with_memory_space_constraint(operand, pltpu.HBM)
                for operand in (
                    tokens,
                    jnp.transpose(gate_weight, (0, 2, 1)),
                    jnp.transpose(up_weight, (0, 2, 1)),
                    down_weight,
                    router_weight.T,
                    carry_mean.reshape(width // LANES, LANES),
                )
            )
        )

    placed = (
        P("dp", None),
        P(None, "dp", "tensor"),
        P(None, "dp", "tensor"),
        P(None, "tensor", "dp"),
        P(),
        P(),
    )
    return jax.shard_map(
        on_device, mesh=mesh, in_specs=placed, out_specs=P(("dp", "tensor"), None), check_vma=False
    )
```

```python
import functools

import jax
import jax.numpy as jnp
from jax import lax
from jax.experimental import pallas as pl
from jax.experimental.pallas import tpu as pltpu
from jax.sharding import PartitionSpec as P

MESH = pl.DeviceIdType.MESH
SEG = 256
CAP = 8.0
NX = 4
LANES = 128
STEP = 32

READY = (
    ((2, 2), (1, 2), (2, 1), (2, 3), (1, 1), (1, 3), (2, 0), (0, 2)),
    ((3, 2), (3, 1), (3, 3), (3, 0), (0, 1), (0, 3), (1, 0), (0, 0)),
)
OFFSETS = tuple(o for group in READY for o in group if o != (0, 0))
NEAR = tuple(o for o in OFFSETS if o != (2, 2))
ALL = OFFSETS + ((0, 0),)
SLOTS = (((0, 0), (1, 2), (0, 2), (1, 0)), ((0, 1), (1, 3), (0, 3)), ((1, 1),))
DIRECT = (2,)
FIRST = tuple(sum(len(group) for group in SLOTS[:g]) for g in range(len(SLOTS) + 1))


def kernel(
    n_dp, n_tensor,
    tok_h, gate_h, up_h, down_h, router_h, carry_h, out_ref,
    tok, weights, router, carry, row_out, row_in, merged, recv, recv_dn,
    acc_g, acc_u, hid, part, via_in, via_out, red_in,
    load_sem, row_send, row_recv, gu_send, gu_recv, dn_send, dn_recv, own_send, own_recv,
    hid_send, hid_recv, via_send, via_recv, red_send, red_recv, round_sem,
):
    d = lax.axis_index("dp")
    t = lax.axis_index("tensor")
    n_y = n_dp // NX
    n_z = n_tensor // 2
    x, y = lax.rem(d, NX), lax.div(d, NX)
    c, z = lax.rem(t, 2), lax.div(t, 2)
    q = lax.rem(x + c, 2)
    experts = weights.shape[0]
    ff = gate_h.shape[1]

    def peer(dx, dy):
        return lax.rem(y + dy, n_y) * NX + lax.rem(x + dx, NX)

    def source(dx, dy):
        return lax.rem(y + n_y - dy, n_y) * NX + lax.rem(x + NX - dx, NX)

    def z_at(offset):
        return lax.rem(z + offset + n_z, n_z)

    sibling = z * 2 + 1 - c

    def copy_to(src, dst, send, recv_sem, dp=None, tensor=None):
        to = {}
        if dp is not None:
            to["dp"] = dp
        if tensor is not None:
            to["tensor"] = tensor
        return pltpu.make_async_remote_copy(
            src_ref=src, dst_ref=dst, send_sem=send, recv_sem=recv_sem,
            device_id=to, device_id_type=MESH,
        )

    def wait_all(ref, sem):
        pltpu.make_async_copy(ref, ref, sem).wait()

    loads = [
        pltpu.make_async_copy(router_h, router, load_sem.at[0]),
        pltpu.make_async_copy(carry_h, carry, load_sem.at[1]),
        pltpu.make_async_copy(tok_h, tok, load_sem.at[2]),
        pltpu.make_async_copy(gate_h, weights.at[:, 0:ff, :], load_sem.at[3]),
        pltpu.make_async_copy(up_h, weights.at[:, ff : 2 * ff, :], load_sem.at[3]),
        pltpu.make_async_copy(down_h, weights.at[:, 2 * ff : 3 * ff, :], load_sem.at[3]),
    ]
    for load in loads:
        load.start()

    barrier = pltpu.get_barrier_semaphore()
    for dx, dy in OFFSETS:
        pl.semaphore_signal(barrier, inc=1, device_id={"dp": peer(dx, dy)}, device_id_type=MESH)
    neighbours = [z_at(1) * 2 + c, z_at(-1) * 2 + c]
    for tensor in [sibling] + neighbours:
        pl.semaphore_signal(barrier, inc=1, device_id={"tensor": tensor}, device_id_type=MESH)

    width = experts * STEP
    spread = lax.broadcasted_iota(jnp.int32, (experts, width), 1) // STEP == lax.broadcasted_iota(
        jnp.int32, (experts, width), 0
    )
    for load in loads[:3]:
        load.wait()
    acc = jnp.zeros((experts, LANES), jnp.float32)
    for i in range(tok.shape[1] // LANES):
        block = tok[:, i * LANES : (i + 1) * LANES].astype(jnp.float32)
        mean = jnp.sum(block, axis=0, keepdims=True) / SEG
        mean = jnp.where(d == n_dp - 1, carry[i : i + 1, :], mean)
        acc += router[:, i * LANES : (i + 1) * LANES] * mean
    total = jnp.sum(acc, axis=1, keepdims=True)
    logits = CAP * jnp.tanh(total / CAP)
    scores = jnp.exp(logits)
    probs = scores / jnp.sum(scores, axis=0, keepdims=True)
    probs = probs.astype(jnp.bfloat16).astype(jnp.float32)
    own_row = jnp.sum(jnp.where(spread, probs, 0.0), axis=0, keepdims=True)
    row_out[...] = own_row
    row_in[d] = own_row

    pl.semaphore_wait(barrier, len(OFFSETS) + 3)

    for dx, dy in OFFSETS:
        copy_to(row_out, row_in.at[d], row_send, row_recv.at[int((dx, dy) == (2, 2))], dp=peer(dx, dy)).start()
    wait_all(weights, load_sem.at[3])

    diag = lax.rem(lax.broadcasted_iota(jnp.int32, (STEP, width), 1), STEP) == lax.broadcasted_iota(
        jnp.int32, (STEP, width), 0
    )

    def merge(left, first, start):
        count = left.shape[0] // STEP
        right = weights[:, start : start + STEP, :].reshape(width, LANES)
        both = jnp.dot(left, right, preferred_element_type=jnp.float32)
        merged[first : first + count, start : start + STEP, :] = both.astype(jnp.bfloat16).reshape(
            count, STEP, LANES
        )

    lefts = []
    for order, group in enumerate(READY):
        wait_all(row_in.at[0 : len(NEAR) if order == 0 else 1], row_recv.at[order])
        left = []
        for dx, dy in group:
            src = lax.rem(peer(dx, dy) + n_dp - 1, n_dp)
            left.append(jnp.where(diag, row_in[src], 0.0).astype(jnp.bfloat16))
        left = jnp.concatenate(left, axis=0)
        first = ALL.index(group[0])
        lefts.append((left, first))
        for start in range(0, 2 * ff, STEP):
            merge(left, first, start)
        for offset in group:
            if offset == (0, 0):
                continue
            j = OFFSETS.index(offset)
            copy_to(
                merged.at[j, 0 : 2 * ff, :], recv.at[j], gu_send, gu_recv.at[(j + 1) // 4],
                dp=peer(*offset),
            ).start()

    starts = list(range(2 * ff, 3 * ff - STEP + 1, STEP))
    if starts[-1] + STEP < 3 * ff:
        starts.append(3 * ff - STEP)
    for left, first in lefts:
        for start in starts:
            merge(left, first, start)
    own_at = len(OFFSETS)
    half_rows = pl.ds(pl.multiple_of(c * ff, 16), ff)
    for g, group in enumerate(SLOTS):
        for s, (a, dy) in enumerate(group):
            for dx in (2 * a, 2 * a + 1):
                if (dx, dy) == (0, 0):
                    continue
                copy_to(
                    merged.at[OFFSETS.index((dx, dy)), 2 * ff : 3 * ff, :],
                    recv_dn.at[FIRST[g] + s, half_rows, :],
                    dn_send, dn_recv.at[g],
                    dp=peer(dx, dy), tensor=z * 2 + lax.rem(x, 2),
                ).start()
    own_copy = copy_to(
        merged.at[own_at, 2 * ff : 3 * ff, :], recv_dn.at[0, half_rows, :],
        own_send, own_recv, tensor=sibling,
    )

    @pl.when(q == 1)
    def _():
        own_copy.start()

    @pl.when(q == 0)
    def _():
        recv_dn[0, half_rows, :] = merged[own_at, 2 * ff : 3 * ff, :]

    order = [own_at] + list(range(len(OFFSETS)))
    nt = (((1,), (1,)), ((), ()))
    for g in range(0, len(order), 4):
        first, last = max(g, 1) - 1, min(g + 3, len(OFFSETS))
        for tensor in neighbours:
            pl.semaphore_signal(
                round_sem.at[g // 4], inc=1, device_id={"tensor": tensor}, device_id_type=MESH
            )
        wait_all(recv.at[first:last], gu_recv.at[g // 4])
        left, right_g, right_u = [], [], []
        for j in order[g : g + 4]:
            if j == own_at:
                src, block = d, merged.at[own_at]
            else:
                src, block = source(*OFFSETS[j]), recv.at[j]
            left.append(tok[:, pl.ds(pl.multiple_of(src * LANES, LANES), LANES)])
            right_g.append(block[0:ff, :])
            right_u.append(block[ff : 2 * ff, :])
        left = jnp.concatenate(left, axis=1)
        more_g = lax.dot_general(
            left, jnp.concatenate(right_g, axis=1), nt, preferred_element_type=jnp.float32
        )
        more_u = lax.dot_general(
            left, jnp.concatenate(right_u, axis=1), nt, preferred_element_type=jnp.float32
        )
        if g == 0:
            acc_g[...] = more_g
            acc_u[...] = more_u
        else:
            acc_g[...] += more_g
            acc_u[...] += more_u
        pl.semaphore_wait(round_sem.at[g // 4], 2)
    gate = acc_g[...]
    hid[c] = (gate / (1.0 + jnp.exp(-gate)) * acc_u[...]).astype(jnp.bfloat16)
    swap = copy_to(hid.at[c], hid.at[c], hid_send, hid_recv, tensor=sibling)
    swap.start()
    swap.wait_recv()

    block = part.shape[1]
    n_groups = len(SLOTS)
    spans = [slice(FIRST[g] * LANES, FIRST[g + 1] * LANES) for g in range(n_groups)]
    places = [2 * n_z - 2 if g in DIRECT else 8 for g in range(n_groups)]

    def to_owner(g, n, buffer, row, chip, core):
        copy_to(
            buffer.at[row, :, spans[g]], red_in.at[1 + 2 * n + c, :, spans[g]],
            red_send.at[g], red_recv.at[g],
            tensor=z_at(chip) * 2 + core,
        ).start()

    def begin(g):
        if g == 0:

            @pl.when(q == 0)
            def _():
                wait_all(recv_dn.at[0, half_rows, :], own_recv)
                wait_all(recv_dn.at[1 : FIRST[1]], dn_recv.at[0])

            @pl.when(q == 1)
            def _():
                wait_all(recv_dn.at[0 : FIRST[1]], dn_recv.at[0])

        else:
            wait_all(recv_dn.at[FIRST[g] : FIRST[g + 1]], dn_recv.at[g])
        term = None
        for core in range(2):
            right = jnp.concatenate(
                [recv_dn[s, core * ff : (core + 1) * ff, :] for s in range(FIRST[g], FIRST[g + 1])],
                axis=1,
            )
            more = jnp.dot(hid[core], right, preferred_element_type=jnp.float32)
            term = more if term is None else term + more
        part[:, :, spans[g]] = term.astype(jnp.bfloat16).reshape(n_tensor, block, -1)
        if g in DIRECT:
            ways = (4, 3, -3, 2, -2, 1, -1)
        else:
            for n, owner, hops in ((2, 4, 2 - 4 * (g % 2)), (0, 3, 1), (1, -3, -1)):
                rows_at = pl.ds(pl.multiple_of(z_at(owner) * 2, 2), 2)
                copy_to(
                    part.at[rows_at, :, spans[g]], via_in.at[n, :, :, spans[g]],
                    via_send.at[g], via_recv.at[g], tensor=z_at(hops) * 2 + c,
                ).start()
            ways = (1, -1)
        for n, way in enumerate(ways):
            for core in (0, 1):
                to_owner(g, n, part, z_at(way) * 2 + core, way, core)
        copy_to(
            part.at[sibling, :, spans[g]], red_in.at[0, :, spans[g]],
            red_send.at[g], red_recv.at[g], tensor=sibling,
        ).start()

    def relay(g):
        wait_all(via_in.at[:, :, :, spans[g]], via_recv.at[g])
        for n, way in ((0, 1), (1, -1)):
            rows_at = pl.ds(pl.multiple_of(z_at(2 * way) * 2, 2), 2)
            value = part[rows_at, :, spans[g]].astype(jnp.float32)
            value = value + via_in[n, :, :, spans[g]].astype(jnp.float32)
            if n == g % 2:
                value = value + via_in[2, :, :, spans[g]].astype(jnp.float32)
            via_out[n, :, :, spans[g]] = value.astype(jnp.bfloat16)
            for core in (0, 1):
                to_owner(g, 2 + n, via_out.at[n], core, 2 * way, core)

    def finish(g):
        wait_all(red_in.at[0 : 1 + places[g], :, spans[g]], red_recv.at[g])
        for of in range(2):
            core = c if of == 0 else 1 - c
            value = part[t, :, spans[g]] if of == 0 else red_in[0, :, spans[g]]
            value = value.astype(jnp.float32)
            for n in range(places[g] // 2):
                value = value + red_in[1 + 2 * n + core, :, spans[g]].astype(jnp.float32)
            odd = lax.rem(x + core, 2)
            for s, (a, dy) in enumerate(SLOTS[g]):
                src = source(2 * a + odd, dy)
                out_ref[:, pl.ds(pl.multiple_of(src * LANES, LANES), LANES)] = value[
                    :, s * LANES : (s + 1) * LANES
                ].astype(jnp.bfloat16)

    for g in range(n_groups):
        begin(g)
    for g in range(n_groups):
        if g not in DIRECT:
            relay(g)
    for g in range(n_groups):
        finish(g)

    peers = len(OFFSETS)
    wait_all(row_in.at[0:peers], row_send)
    wait_all(merged.at[0:peers, 0 : 2 * ff, :], gu_send)
    wait_all(merged.at[0:peers, 2 * ff : 3 * ff, :], dn_send)
    for g in range(n_groups):
        if g not in DIRECT:
            wait_all(via_in.at[:, :, :, spans[g]], via_send.at[g])
        wait_all(red_in.at[0 : 1 + places[g], :, spans[g]], red_send.at[g])

    @pl.when(q == 1)
    def _():
        own_copy.wait_send()

    swap.wait_send()


def solution(mesh):
    n_dp, n_tensor = mesh.shape["dp"], mesh.shape["tensor"]

    def on_device(tokens, gate_weight, up_weight, down_weight, router_weight, carry_mean):
        rows, width = tokens.shape
        experts, _, ff = gate_weight.shape
        peers = len(OFFSETS)
        groups = len(SLOTS)
        block = rows // n_tensor
        slots = FIRST[-1]
        cols = slots * LANES
        bf16, f32 = jnp.bfloat16, jnp.float32
        dma = pltpu.SemaphoreType.DMA
        return pl.pallas_call(
            functools.partial(kernel, n_dp, n_tensor),
            out_shape=jax.ShapeDtypeStruct((block, width), bf16),
            in_specs=[pl.BlockSpec(memory_space=pltpu.HBM)] * 6,
            out_specs=pl.BlockSpec(memory_space=pltpu.VMEM),
            scratch_shapes=[
                pltpu.VMEM((rows, width), bf16),
                pltpu.VMEM((experts, 3 * ff, LANES), bf16),
                pltpu.VMEM((experts, width), f32),
                pltpu.VMEM((width // LANES, LANES), f32),
                pltpu.VMEM((1, experts * STEP), f32),
                pltpu.VMEM((n_dp, 1, experts * STEP), f32),
                pltpu.VMEM((n_dp, 3 * ff, LANES), bf16),
                pltpu.VMEM((peers, 2 * ff, LANES), bf16),
                pltpu.VMEM((slots, 2 * ff, LANES), bf16),
                pltpu.VMEM((rows, ff), f32),
                pltpu.VMEM((rows, ff), f32),
                pltpu.VMEM((2, rows, ff), bf16),
                pltpu.VMEM((n_tensor, block, cols), bf16),
                pltpu.VMEM((3, 2, block, cols), bf16),
                pltpu.VMEM((2, 2, block, cols), bf16),
                pltpu.VMEM((n_tensor - 1, block, cols), bf16),
                dma((4,)),
                dma(()), dma((2,)),
                dma(()), dma((4,)),
                dma(()), dma((groups,)), dma(()), dma(()),
                dma(()), dma(()),
                dma((groups,)), dma((groups,)),
                dma((groups,)), dma((groups,)),
                pltpu.SemaphoreType.REGULAR((4,)),
            ],
            compiler_params=pltpu.CompilerParams(
                collective_id=0, has_side_effects=True, vmem_limit_bytes=32 << 20
            ),
        )(
            *(
                pltpu.with_memory_space_constraint(operand, pltpu.HBM)
                for operand in (
                    tokens,
                    jnp.transpose(gate_weight, (0, 2, 1)),
                    jnp.transpose(up_weight, (0, 2, 1)),
                    down_weight,
                    router_weight.T,
                    carry_mean.reshape(width // LANES, LANES),
                )
            )
        )

    placed = (
        P("dp", None),
        P(None, "dp", "tensor"),
        P(None, "dp", "tensor"),
        P(None, "tensor", "dp"),
        P(),
        P(),
    )
    return jax.shard_map(
        on_device, mesh=mesh, in_specs=placed, out_specs=P(("dp", "tensor"), None), check_vma=False
    )
```

```python
import functools

import jax
import jax.numpy as jnp
from jax import lax
from jax.experimental import pallas as pl
from jax.experimental.pallas import tpu as pltpu
from jax.sharding import PartitionSpec as P

MESH = pl.DeviceIdType.MESH
SEG = 256
CAP = 8.0
NX = 4
LANES = 128
STEP = 32

READY = (
    ((2, 2), (1, 2), (2, 1), (2, 3), (1, 1), (1, 3), (2, 0), (0, 2)),
    ((3, 2), (3, 1), (3, 3), (3, 0), (0, 1), (0, 3), (1, 0), (0, 0)),
)
OFFSETS = tuple(o for group in READY for o in group if o != (0, 0))
NEAR = tuple(o for o in OFFSETS if o != (2, 2))
ALL = OFFSETS + ((0, 0),)
SLOTS = (((0, 0), (1, 2), (0, 2), (1, 0)), ((0, 1), (1, 3), (0, 3)), ((1, 1),))
DIRECT = (2,)
FIRST = tuple(sum(len(group) for group in SLOTS[:g]) for g in range(len(SLOTS) + 1))


def kernel(
    n_dp, n_tensor,
    tok_h, gate_h, up_h, down_h, router_h, carry_h, out_ref,
    tok, weights, router, carry, row_out, row_in, merged, recv, recv_dn,
    acc_g, acc_u, hid, part, via_in, via_out, red_in,
    load_sem, row_send, row_recv, gu_send, gu_recv, dn_send, dn_recv, own_send, own_recv,
    hid_send, hid_recv, via_send, via_recv, red_send, red_recv, round_sem,
):
    d = lax.axis_index("dp")
    t = lax.axis_index("tensor")
    n_y = n_dp // NX
    n_z = n_tensor // 2
    x, y = lax.rem(d, NX), lax.div(d, NX)
    c, z = lax.rem(t, 2), lax.div(t, 2)
    q = lax.rem(x + c, 2)
    experts = weights.shape[0]
    ff = gate_h.shape[1]

    def peer(dx, dy):
        return lax.rem(y + dy, n_y) * NX + lax.rem(x + dx, NX)

    def source(dx, dy):
        return lax.rem(y + n_y - dy, n_y) * NX + lax.rem(x + NX - dx, NX)

    def z_at(offset):
        return lax.rem(z + offset + n_z, n_z)

    sibling = z * 2 + 1 - c

    def copy_to(src, dst, send, recv_sem, dp=None, tensor=None):
        to = {}
        if dp is not None:
            to["dp"] = dp
        if tensor is not None:
            to["tensor"] = tensor
        return pltpu.make_async_remote_copy(
            src_ref=src, dst_ref=dst, send_sem=send, recv_sem=recv_sem,
            device_id=to, device_id_type=MESH,
        )

    def wait_all(ref, sem):
        pltpu.make_async_copy(ref, ref, sem).wait()

    loads = [
        pltpu.make_async_copy(router_h, router, load_sem.at[0]),
        pltpu.make_async_copy(carry_h, carry, load_sem.at[1]),
        pltpu.make_async_copy(tok_h, tok, load_sem.at[2]),
        pltpu.make_async_copy(gate_h, weights.at[:, 0:ff, :], load_sem.at[3]),
        pltpu.make_async_copy(up_h, weights.at[:, ff : 2 * ff, :], load_sem.at[3]),
        pltpu.make_async_copy(down_h, weights.at[:, 2 * ff : 3 * ff, :], load_sem.at[3]),
    ]
    barrier = pltpu.get_barrier_semaphore()
    for dx, dy in OFFSETS:
        pl.semaphore_signal(barrier, inc=1, device_id={"dp": peer(dx, dy)}, device_id_type=MESH)
    neighbours = [z_at(1) * 2 + c, z_at(-1) * 2 + c]
    for tensor in [sibling] + neighbours:
        pl.semaphore_signal(barrier, inc=1, device_id={"tensor": tensor}, device_id_type=MESH)

    for load in loads:
        load.start()

    width = experts * STEP
    spread = lax.broadcasted_iota(jnp.int32, (experts, width), 1) // STEP == lax.broadcasted_iota(
        jnp.int32, (experts, width), 0
    )
    for load in loads[:3]:
        load.wait()
    acc = jnp.zeros((experts, LANES), jnp.float32)
    for i in range(tok.shape[1] // LANES):
        block = tok[:, i * LANES : (i + 1) * LANES].astype(jnp.float32)
        mean = jnp.sum(block, axis=0, keepdims=True) / SEG
        mean = jnp.where(d == n_dp - 1, carry[i : i + 1, :], mean)
        acc += router[:, i * LANES : (i + 1) * LANES] * mean
    total = jnp.sum(acc, axis=1, keepdims=True)
    logits = CAP * jnp.tanh(total / CAP)
    scores = jnp.exp(logits)
    probs = scores / jnp.sum(scores, axis=0, keepdims=True)
    probs = probs.astype(jnp.bfloat16).astype(jnp.float32)
    own_row = jnp.sum(jnp.where(spread, probs, 0.0), axis=0, keepdims=True)
    row_out[...] = own_row
    row_in[d] = own_row

    pl.semaphore_wait(barrier, len(OFFSETS) + 3)

    for dx, dy in OFFSETS:
        copy_to(row_out, row_in.at[d], row_send, row_recv.at[int((dx, dy) == (2, 2))], dp=peer(dx, dy)).start()
    wait_all(weights, load_sem.at[3])

    diag = lax.rem(lax.broadcasted_iota(jnp.int32, (STEP, width), 1), STEP) == lax.broadcasted_iota(
        jnp.int32, (STEP, width), 0
    )

    def merge(left, first, starts):
        count = left.shape[0] // STEP
        right = [weights[:, s : s + STEP, :].reshape(width, LANES) for s in starts]
        both = jnp.dot(left, jnp.concatenate(right, axis=1), preferred_element_type=jnp.float32)
        both = both.astype(jnp.bfloat16).reshape(count, STEP, -1)
        for i, s in enumerate(starts):
            merged[first : first + count, s : s + STEP, :] = both[
                :, :, i * LANES : (i + 1) * LANES
            ]

    lefts = []
    for order, group in enumerate(READY):
        wait_all(row_in.at[0 : len(NEAR) if order == 0 else 1], row_recv.at[order])
        left = []
        for dx, dy in group:
            src = lax.rem(peer(dx, dy) + n_dp - 1, n_dp)
            left.append(jnp.where(diag, row_in[src], 0.0).astype(jnp.bfloat16))
        left = jnp.concatenate(left, axis=0)
        first = ALL.index(group[0])
        lefts.append((left, first))
        for start in range(0, 2 * ff, 2 * STEP):
            merge(left, first, range(start, min(start + 2 * STEP, 2 * ff), STEP))
        for offset in group:
            if offset == (0, 0):
                continue
            j = OFFSETS.index(offset)
            copy_to(
                merged.at[j, 0 : 2 * ff, :], recv.at[j], gu_send, gu_recv.at[(j + 1) // 4],
                dp=peer(*offset),
            ).start()

    starts = list(range(2 * ff, 3 * ff - STEP + 1, STEP))
    if starts[-1] + STEP < 3 * ff:
        starts.append(3 * ff - STEP)
    for left, first in lefts:
        for i in range(0, len(starts), 2):
            merge(left, first, starts[i : i + 2])
    own_at = len(OFFSETS)
    half_rows = pl.ds(pl.multiple_of(c * ff, 16), ff)
    for g, group in enumerate(SLOTS):
        for s, (a, dy) in enumerate(group):
            for dx in (2 * a, 2 * a + 1):
                if (dx, dy) == (0, 0):
                    continue
                copy_to(
                    merged.at[OFFSETS.index((dx, dy)), 2 * ff : 3 * ff, :],
                    recv_dn.at[FIRST[g] + s, half_rows, :],
                    dn_send, dn_recv.at[g],
                    dp=peer(dx, dy), tensor=z * 2 + lax.rem(x, 2),
                ).start()
    own_copy = copy_to(
        merged.at[own_at, 2 * ff : 3 * ff, :], recv_dn.at[0, half_rows, :],
        own_send, own_recv, tensor=sibling,
    )

    @pl.when(q == 1)
    def _():
        own_copy.start()

    @pl.when(q == 0)
    def _():
        recv_dn[0, half_rows, :] = merged[own_at, 2 * ff : 3 * ff, :]

    order = [own_at] + list(range(len(OFFSETS)))
    nt = (((1,), (1,)), ((), ()))
    for g in range(0, len(order), 4):
        first, last = max(g, 1) - 1, min(g + 3, len(OFFSETS))
        for tensor in neighbours:
            pl.semaphore_signal(
                round_sem.at[g // 4], inc=1, device_id={"tensor": tensor}, device_id_type=MESH
            )
        wait_all(recv.at[first:last], gu_recv.at[g // 4])
        left, right_g, right_u = [], [], []
        for j in order[g : g + 4]:
            if j == own_at:
                src, block = d, merged.at[own_at]
            else:
                src, block = source(*OFFSETS[j]), recv.at[j]
            left.append(tok[:, pl.ds(pl.multiple_of(src * LANES, LANES), LANES)])
            right_g.append(block[0:ff, :])
            right_u.append(block[ff : 2 * ff, :])
        left = jnp.concatenate(left, axis=1)
        more_g = lax.dot_general(
            left, jnp.concatenate(right_g, axis=1), nt, preferred_element_type=jnp.float32
        )
        more_u = lax.dot_general(
            left, jnp.concatenate(right_u, axis=1), nt, preferred_element_type=jnp.float32
        )
        if g == 0:
            acc_g[...] = more_g
            acc_u[...] = more_u
        else:
            acc_g[...] += more_g
            acc_u[...] += more_u
        pl.semaphore_wait(round_sem.at[g // 4], 2)
    gate = acc_g[...]
    hid[c] = (gate / (1.0 + jnp.exp(-gate)) * acc_u[...]).astype(jnp.bfloat16)
    swap = copy_to(hid.at[c], hid.at[c], hid_send, hid_recv, tensor=sibling)
    swap.start()
    swap.wait_recv()

    block = part.shape[1]
    n_groups = len(SLOTS)
    spans = [slice(FIRST[g] * LANES, FIRST[g + 1] * LANES) for g in range(n_groups)]
    places = [2 * n_z - 2 if g in DIRECT else 8 for g in range(n_groups)]

    def to_owner(g, n, buffer, row, chip, core):
        copy_to(
            buffer.at[row, :, spans[g]], red_in.at[1 + 2 * n + c, :, spans[g]],
            red_send.at[g], red_recv.at[g],
            tensor=z_at(chip) * 2 + core,
        ).start()

    def begin(g):
        if g == 0:

            @pl.when(q == 0)
            def _():
                wait_all(recv_dn.at[0, half_rows, :], own_recv)
                wait_all(recv_dn.at[1 : FIRST[1]], dn_recv.at[0])

            @pl.when(q == 1)
            def _():
                wait_all(recv_dn.at[0 : FIRST[1]], dn_recv.at[0])

        else:
            wait_all(recv_dn.at[FIRST[g] : FIRST[g + 1]], dn_recv.at[g])
        term = None
        for core in range(2):
            right = jnp.concatenate(
                [recv_dn[s, core * ff : (core + 1) * ff, :] for s in range(FIRST[g], FIRST[g + 1])],
                axis=1,
            )
            more = jnp.dot(hid[core], right, preferred_element_type=jnp.float32)
            term = more if term is None else term + more
        part[:, :, spans[g]] = term.astype(jnp.bfloat16).reshape(n_tensor, block, -1)
        if g in DIRECT:
            ways = (4, 3, -3, 2, -2, 1, -1)
        else:
            for n, owner, hops in ((2, 4, 2 - 4 * (g % 2)), (0, 3, 1), (1, -3, -1)):
                rows_at = pl.ds(pl.multiple_of(z_at(owner) * 2, 2), 2)
                copy_to(
                    part.at[rows_at, :, spans[g]], via_in.at[n, :, :, spans[g]],
                    via_send.at[g], via_recv.at[g], tensor=z_at(hops) * 2 + c,
                ).start()
            ways = (1, -1)
        for n, way in enumerate(ways):
            for core in (0, 1):
                to_owner(g, n, part, z_at(way) * 2 + core, way, core)
        copy_to(
            part.at[sibling, :, spans[g]], red_in.at[0, :, spans[g]],
            red_send.at[g], red_recv.at[g], tensor=sibling,
        ).start()

    def relay(g):
        wait_all(via_in.at[:, :, :, spans[g]], via_recv.at[g])
        for n, way in ((0, 1), (1, -1)):
            rows_at = pl.ds(pl.multiple_of(z_at(2 * way) * 2, 2), 2)
            value = part[rows_at, :, spans[g]].astype(jnp.float32)
            value = value + via_in[n, :, :, spans[g]].astype(jnp.float32)
            if n == g % 2:
                value = value + via_in[2, :, :, spans[g]].astype(jnp.float32)
            via_out[n, :, :, spans[g]] = value.astype(jnp.bfloat16)
            for core in (0, 1):
                to_owner(g, 2 + n, via_out.at[n], core, 2 * way, core)

    def finish(g):
        wait_all(red_in.at[0 : 1 + places[g], :, spans[g]], red_recv.at[g])
        for of in range(2):
            core = c if of == 0 else 1 - c
            value = part[t, :, spans[g]] if of == 0 else red_in[0, :, spans[g]]
            value = value.astype(jnp.float32)
            for n in range(places[g] // 2):
                value = value + red_in[1 + 2 * n + core, :, spans[g]].astype(jnp.float32)
            odd = lax.rem(x + core, 2)
            for s, (a, dy) in enumerate(SLOTS[g]):
                src = source(2 * a + odd, dy)
                out_ref[:, pl.ds(pl.multiple_of(src * LANES, LANES), LANES)] = value[
                    :, s * LANES : (s + 1) * LANES
                ].astype(jnp.bfloat16)

    for g in range(n_groups):
        begin(g)
    for g in range(n_groups):
        if g not in DIRECT:
            relay(g)
    for g in range(n_groups):
        finish(g)

    peers = len(OFFSETS)
    wait_all(row_in.at[0:peers], row_send)
    wait_all(merged.at[0:peers, 0 : 2 * ff, :], gu_send)
    wait_all(merged.at[0:peers, 2 * ff : 3 * ff, :], dn_send)
    for g in range(n_groups):
        if g not in DIRECT:
            wait_all(via_in.at[:, :, :, spans[g]], via_send.at[g])
        wait_all(red_in.at[0 : 1 + places[g], :, spans[g]], red_send.at[g])

    @pl.when(q == 1)
    def _():
        own_copy.wait_send()

    swap.wait_send()


def solution(mesh):
    n_dp, n_tensor = mesh.shape["dp"], mesh.shape["tensor"]

    def on_device(tokens, gate_weight, up_weight, down_weight, router_weight, carry_mean):
        rows, width = tokens.shape
        experts, _, ff = gate_weight.shape
        peers = len(OFFSETS)
        groups = len(SLOTS)
        block = rows // n_tensor
        slots = FIRST[-1]
        cols = slots * LANES
        bf16, f32 = jnp.bfloat16, jnp.float32
        dma = pltpu.SemaphoreType.DMA
        return pl.pallas_call(
            functools.partial(kernel, n_dp, n_tensor),
            out_shape=jax.ShapeDtypeStruct((block, width), bf16),
            in_specs=[pl.BlockSpec(memory_space=pltpu.HBM)] * 6,
            out_specs=pl.BlockSpec(memory_space=pltpu.VMEM),
            scratch_shapes=[
                pltpu.VMEM((rows, width), bf16),
                pltpu.VMEM((experts, 3 * ff, LANES), bf16),
                pltpu.VMEM((experts, width), f32),
                pltpu.VMEM((width // LANES, LANES), f32),
                pltpu.VMEM((1, experts * STEP), f32),
                pltpu.VMEM((n_dp, 1, experts * STEP), f32),
                pltpu.VMEM((n_dp, 3 * ff, LANES), bf16),
                pltpu.VMEM((peers, 2 * ff, LANES), bf16),
                pltpu.VMEM((slots, 2 * ff, LANES), bf16),
                pltpu.VMEM((rows, ff), f32),
                pltpu.VMEM((rows, ff), f32),
                pltpu.VMEM((2, rows, ff), bf16),
                pltpu.VMEM((n_tensor, block, cols), bf16),
                pltpu.VMEM((3, 2, block, cols), bf16),
                pltpu.VMEM((2, 2, block, cols), bf16),
                pltpu.VMEM((n_tensor - 1, block, cols), bf16),
                dma((4,)),
                dma(()), dma((2,)),
                dma(()), dma((4,)),
                dma(()), dma((groups,)), dma(()), dma(()),
                dma(()), dma(()),
                dma((groups,)), dma((groups,)),
                dma((groups,)), dma((groups,)),
                pltpu.SemaphoreType.REGULAR((4,)),
            ],
            compiler_params=pltpu.CompilerParams(
                collective_id=0, has_side_effects=True, vmem_limit_bytes=32 << 20
            ),
        )(
            *(
                pltpu.with_memory_space_constraint(operand, pltpu.HBM)
                for operand in (
                    tokens,
                    jnp.transpose(gate_weight, (0, 2, 1)),
                    jnp.transpose(up_weight, (0, 2, 1)),
                    down_weight,
                    router_weight.T,
                    carry_mean.reshape(width // LANES, LANES),
                )
            )
        )

    placed = (
        P("dp", None),
        P(None, "dp", "tensor"),
        P(None, "dp", "tensor"),
        P(None, "tensor", "dp"),
        P(),
        P(),
    )
    return jax.shard_map(
        on_device, mesh=mesh, in_specs=placed, out_specs=P(("dp", "tensor"), None), check_vma=False
    )
```
